512 devices in a mesh: row: 32 (over z, x_hi, core), col: 16 (over y, x_lo).
Axes of the slice: x: 4 (x_hi: 2, x_lo: 2; x = x_hi * 2 + x_lo), y: 8, z: 8, core: 2. Of those that a mesh axis runs over, the one named last changes fastest.
Arguments:
- reference_image: float32 [4096, 4096], P('row', 'col'), may hold values from -6 to 6
- source_images: float32 [4, 4096, 4096], P(None, 'row', 'col'), may hold values from -6 to 6
- hypotheses: int32 [8, 4096, 4096], P(None, 'row', 'col'), may hold values from 0 to 15
- source_ids: int32 [4], replicated, may hold values from 1 to 3
- coarse_disp: float32 [512, 512], P('col'), may hold values from 0 to 15
- coarse_conf: float32 [512, 512], P('col'), may hold values from 0.1 to 10
Outputs:
- disparity: float32 [4096, 4096], P('row', 'col')
The draws below stay inside these ranges and needn't reach their ends.
All inputs are finite; a program needn't handle non-finite values.
Results may differ from the reference program's by a relative error of at most 0.0003.
Values sent between devices are 32-bit elements; how exact they have to be, the bound alone decides.
A program may use at most 64 MiB of HBM per device.

```python
import math
import jax
import jax.numpy as jnp
from jax import lax

LEVELS = 16
HYP = 8
SRC = 4
MAXID = 3
WIN = 11
UPS = 8
CITER = 4
H = 4096
W = 4096
CH = 512
CW = 512


def plant(array, own_key, smallest, top_value):
    shape = array.shape
    spot = [jax.random.randint(jax.random.fold_in(own_key, axis), (), 0, shape[axis]) for axis in range(len(shape))]
    array = array.at[tuple(spot)].set(smallest)
    longest = shape.index(max(shape))
    spot[longest] = (spot[longest] + 1) % shape[longest]
    return array.at[tuple(spot)].set(top_value)


def levels(key, dims, cuts, low, high):
    factor_of, own = 1.0, jax.random.fold_in(key, 6)
    for position, shards_of in cuts:
        steps = jnp.exp(jax.random.uniform(jax.random.fold_in(own, position), (shards_of,), jnp.float32, low / len(cuts), high / len(cuts)))
        factor_of = factor_of * jnp.repeat(steps, dims[position] // shards_of).reshape([-1 if axis == position else 1 for axis in range(len(dims))])
    return factor_of


def bell_draw(stream_key, shape, scale, bound, pieces=(), held_as=jnp.bfloat16):
    values = scale * jax.random.normal(stream_key, shape, jnp.float32)
    if pieces:
        values = values * levels(stream_key, shape, pieces, -0.22, 0.18)
    return jnp.clip(values, -bound, bound).astype(held_as)


def setup_inputs(seed: int = 0) -> dict:
    keys = jax.random.split(jax.random.key(seed), 7)
    return {
        "reference_image": bell_draw(keys[0], (H, W), 1.0, 6.0, ((0, 32), (1, 16)), jnp.float32),
        "source_images": bell_draw(keys[1], (SRC, H, W), 1.0, 6.0, ((1, 32), (2, 16)), jnp.float32),
        "hypotheses": plant(jax.random.randint(keys[2], (HYP, H, W), 0, LEVELS), jax.random.fold_in(keys[2], 1), 0, LEVELS - 1).astype(jnp.int32),
        "source_ids": plant(jax.random.randint(keys[3], (SRC,), 1, MAXID + 1), jax.random.fold_in(keys[3], 1), 1, MAXID).astype(jnp.int32),
        "coarse_disp": jnp.clip(15.0 * jax.random.uniform(keys[4], (CH, CW), jnp.float32) ** levels(keys[4], (CH, CW), ((0, 16),), -0.2, 0.2), 0.0, 15.0),
        "coarse_conf": jnp.clip(jnp.exp(math.log(10.0) - 4.6051702 * jax.random.uniform(keys[5], (CH, CW), jnp.float32) ** levels(keys[5], (CH, CW), ((0, 16),), -0.2, 0.2)), 0.1, 10.0),
    }


smooth_pull = 1.0
previous_estimate_factor = 0.01
exponential_sharpness = 0.1
variance_floor = 1e-05

def window_sums(values):
    radius = WIN // 2
    widths = [(0, 0)] * (values.ndim - 2) + [(radius, radius), (radius, radius)]
    padded = jnp.pad(values, widths)
    height = values.shape[-2]
    width_cols = values.shape[-1]
    row_sums = padded[..., 0:height, :]
    for offset in range(1, WIN):
        row_sums = row_sums + padded[..., offset:offset + height, :]
    accumulated_sums = row_sums[..., 0:width_cols]
    for offset in range(1, WIN):
        accumulated_sums = accumulated_sums + row_sums[..., offset:offset + width_cols]
    return accumulated_sums

def interp_matrix(fine_start, fine_count, coarse_start, coarse_pixel_number, coarse_total):
    fine_pos = fine_start + jnp.arange(fine_count, dtype=jnp.int32)
    numerator = 2 * fine_pos + 1 - UPS
    lower = numerator // (2 * UPS)
    fraction = (numerator - lower * 2 * UPS).astype(jnp.float32) / (2.0 * UPS)
    low_index = jnp.clip(lower, 0, coarse_total - 1) - coarse_start
    high_index = jnp.clip(lower + 1, 0, coarse_total - 1) - coarse_start
    columns = jnp.arange(coarse_pixel_number, dtype=jnp.int32)
    low_part = jnp.where(columns[None, :] == low_index[:, None], 1.0 - fraction[:, None], 0.0)
    high_part = jnp.where(columns[None, :] == high_index[:, None], fraction[:, None], 0.0)
    return low_part + high_part

def jacobi_step(padded_line_span, disp, conf):
    middle = padded_line_span[1:-1]
    col_pad = jnp.pad(middle, ((0, 0), (1, 1)))
    neighbours = padded_line_span[:-2] + padded_line_span[2:] + col_pad[:, :-2] + col_pad[:, 2:]
    return (conf * disp + smooth_pull * neighbours) / (conf + 4.0 * smooth_pull)

def estimate(chosen_hypothesis, candidate, centre):
    neighbour_jump_cost = 1.0 - chosen_hypothesis + previous_estimate_factor * (candidate - centre[None]) ** 2
    candidate_mixing_shares = jnp.exp(-neighbour_jump_cost / exponential_sharpness)
    return lax.optimization_barrier(jnp.sum(candidate_mixing_shares * candidate, axis=0)) / lax.optimization_barrier(jnp.sum(candidate_mixing_shares, axis=0))

def reference(reference_image, source_images, hypotheses, source_ids, coarse_disp, coarse_conf):
    current = coarse_disp
    for sweep in range(CITER):
        current = jacobi_step(jnp.pad(current, ((1, 1), (0, 0))), coarse_disp, coarse_conf)
    rows_mat = interp_matrix(0, H, 0, CH, CH)
    cols_mat = interp_matrix(0, W, 0, CW, CW)
    upsampled = jnp.dot(jnp.dot(rows_mat, current, precision=lax.Precision.HIGHEST), cols_mat.T, precision=lax.Precision.HIGHEST)
    area = float(WIN * WIN)
    shift_most = MAXID * (LEVELS - 1)
    wide = jnp.pad(source_images, ((0, 0), (0, 0), (shift_most, 0)))
    src_mean = window_sums(wide) / area
    src_var = window_sums(wide * wide) / area - src_mean ** 2 + variance_floor
    ref_mean = window_sums(reference_image) / area
    ref_var = window_sums(reference_image * reference_image) / area - ref_mean ** 2 + variance_floor

    def level_step(chosen_hypothesis, depth_level):
        ncc_sum = jnp.zeros((H, W), jnp.float32)
        for view_slot in range(SRC):
            begin_col = (shift_most - source_ids[view_slot] * depth_level).astype(jnp.int32)
            shifted = lax.dynamic_slice_in_dim(wide[view_slot], begin_col, W, 1)
            cross = window_sums(reference_image * shifted) / area
            mean_src = lax.dynamic_slice_in_dim(src_mean[view_slot], begin_col, W, 1)
            var_src = lax.dynamic_slice_in_dim(src_var[view_slot], begin_col, W, 1)
            ncc_sum = ncc_sum + (cross - ref_mean * mean_src) / jnp.sqrt(ref_var * var_src)
        volume = ncc_sum / SRC
        return (chosen_hypothesis + jnp.where(hypotheses == depth_level, volume[None], 0.0), None)
    chosen_hypothesis, unused = lax.scan(level_step, jnp.zeros((HYP, H, W), jnp.float32), jnp.arange(LEVELS, dtype=jnp.int32))
    candidate = hypotheses.astype(jnp.float32)
    red = estimate(chosen_hypothesis, candidate, upsampled)
    padded_red = jnp.pad(red, 1)
    neighbours = padded_red[:-2, 1:-1] + padded_red[2:, 1:-1] + padded_red[1:-1, :-2] + padded_red[1:-1, 2:]
    row_pos = jnp.arange(H, dtype=jnp.int32)
    col_pos = jnp.arange(W, dtype=jnp.int32)
    vertical_strip_bounds = (row_pos == 0).astype(jnp.float32) + (row_pos == H - 1).astype(jnp.float32)
    col_edges = (col_pos == 0).astype(jnp.float32) + (col_pos == W - 1).astype(jnp.float32)
    counted = 4.0 - vertical_strip_bounds[:, None] - col_edges[None, :]
    centre = 0.5 * upsampled + 0.5 * neighbours / counted
    black = estimate(chosen_hypothesis, candidate, centre)
    parity = (row_pos[:, None] + col_pos[None, :]) % 2 == 0
    return jnp.where(parity, red, black)
```

```python
import functools

import jax
import jax.numpy as jnp
from jax import lax
from jax.experimental import pallas as pl
from jax.experimental.pallas import tpu as pltpu
from jax.sharding import PartitionSpec as P

LEVELS = 16
HYP = 8
SRC = 4
MAXID = 3
WIN = 11
UPS = 8
CITER = 4
R = WIN // 2
AREA = float(WIN * WIN)
FLOOR = 1e-05

ROWS, COLS = 128, 256
SEGS = 8
SEG = COLS // SEGS
SHIFT = MAXID * (LEVELS - 1)
LEFT = SHIFT + R
PADL = 56
CI = 320
NJ = SEG + 2 * R + SHIFT
NK = SEG + 2 * R
NM = SEG + SHIFT
HL = 2 * R
bf16 = jnp.bfloat16
f32 = jnp.float32


def window11(vals):
    n = len(vals)
    count = n - WIN + 1
    suf, pre = {}, {}
    for start in range(0, n, WIN):
        stop = min(start + WIN, n)
        if stop - start == WIN and start < count:
            acc = vals[stop - 1]
            suf[stop - 1] = acc
            for i in range(stop - 2, start - 1, -1):
                acc = vals[i] + acc
                suf[i] = acc
        if start:
            acc = vals[start]
            pre[start] = acc
            for i in range(start + 1, min(stop, start + WIN - 1)):
                acc = acc + vals[i]
                pre[i] = acc
    return [suf[i] if i % WIN == 0 else suf[i] + pre[i + WIN - 1] for i in range(count)]


def parts(value, count):
    out = []
    for _ in range(count - 1):
        piece = value.astype(bf16)
        out.append(piece)
        value = value - piece.astype(f32)
    out.append(value.astype(bf16))
    return out


def put_parts(ref, sums, columns):
    n = len(sums)
    for q in range(0, n, 2):
        both = jnp.concatenate(sums[q:q + 2], axis=0) if q + 1 < n else sums[q]
        for piece, col in zip(parts(both, len(columns)), columns):
            ref[8 * q:8 * q + both.shape[0], col:col + 128] = piece


def band_main():
    a = lax.broadcasted_iota(jnp.int32, (ROWS, ROWS), 0)
    b = lax.broadcasted_iota(jnp.int32, (ROWS, ROWS), 1)
    return jnp.where(jnp.abs(a - b) <= R, 1.0, 0.0).astype(bf16)


def band_halo(view):
    a = lax.broadcasted_iota(jnp.int32, (128, ROWS), 0) - view * HL
    b = lax.broadcasted_iota(jnp.int32, (128, ROWS), 1)
    row = jnp.where(a < R, a - R, a - R + ROWS)
    good = (a >= 0) & (a < HL) & (jnp.abs(row - b) <= R)
    return jnp.where(good, 1.0, 0.0).astype(bf16)


def score_kernel(ids, xm, xh, hyp, up, sel_out, ht_out, red_out,
                 xs, hs, rt, rx3, rmom, xmom, lmom, cmom, av, bv, lhs, lx, yy, vol, htc):
    zero = jnp.zeros((128, 128), bf16)
    b = band_main()
    halo = [band_halo(v) for v in range(SRC)]
    rt[0:128, 0:128] = b
    rt[0:128, 128:256] = zero
    rt[128:256, 0:128] = zero
    rt[128:256, 128:256] = b
    for v in range(SRC):
        rmom[v, 0:128, 0:128] = halo[v]
        rmom[v, 0:128, 128:256] = zero
        rmom[v, 128:256, 0:128] = zero
        rmom[v, 128:256, 128:256] = halo[v]
        p, q = v // 2, v % 2
        rx3[p, 0:128, 128 * q:128 * q + 128] = halo[v]
        rx3[p, 128:256, 128 * q:128 * q + 128] = halo[v]

    for j in range(NJ):
        rows = pl.ds(j + PADL - LEFT, SEGS, stride=SEG)
        for v in range(SRC):
            xs[v + 1, j] = xm[v + 1, rows, :]
        hs[1, j] = xh[1, rows, :]
        if j >= SHIFT:
            xs[0, j] = xm[0, rows, :]
            hs[0, j] = xh[0, rows, :]

    packed = hyp[0]
    for k in range(1, HYP):
        packed = packed | (hyp[k] << (4 * k))
    htc[...] = packed.T
    for i in range(SEG):
        ht_out[8 * i:8 * i + 8, :] = htc[pl.ds(i, SEGS, stride=SEG), :]

    def moments(load, first, count, ref):
        vals = [load(first + j) for j in range(count)]
        put_parts(ref, window11(vals), (0, 256, 512))
        vals = [load(first + j) for j in range(count)]
        put_parts(ref, window11([x * x for x in vals]), (128, 384, 640))

    def finish(rows, view):
        total = jnp.dot(lmom[0:rows, 0:256], rt[...], preferred_element_type=f32)
        for t in (256, 512):
            total += jnp.dot(lmom[0:rows, t:t + 256], rt[...], preferred_element_type=f32)
        for t in (0, 256, 512):
            total += jnp.dot(xmom[0:rows, t:t + 256], rmom[view], preferred_element_type=f32)
        cmom[0:rows, :] = total

    moments(lambda j: hs[0, j], SHIFT, NK, xmom)
    moments(lambda j: xs[0, j], SHIFT, NK, lmom)
    finish(SEG * 8, 0)
    for i in range(SEG):
        m = cmom[8 * i:8 * i + 8, 0:128] / AREA
        var = cmom[8 * i:8 * i + 8, 128:256] / AREA - m * m + FLOOR
        av[0, i] = lax.rsqrt(var)
        bv[0, i] = m

    moments(lambda j: hs[1, j], 0, NJ, xmom)

    def view_moments(v, carry):
        moments(lambda j: xs[v + 1, j], 0, NJ, lmom)
        finish(NM * 8, v)

        def fill(i, c):
            rows = pl.ds(pl.multiple_of(8 * i, 8), 8)
            m = cmom[rows, 0:128] / AREA
            var = cmom[rows, 128:256] / AREA - m * m + FLOOR
            inv = lax.rsqrt(var) / SRC
            av[v + 1, i] = inv / AREA
            bv[v + 1, i] = m * inv
            return c

        return lax.fori_loop(0, NM, fill, carry)

    lax.fori_loop(0, SRC, view_moments, 0)

    lane = lax.broadcasted_iota(jnp.int32, (8, 128), 1)
    masks = [lane < HL * (v + 1) for v in range(SRC - 1)]

    def level(l, carry):
        begins = [SHIFT - ids[v] * l for v in range(SRC)]
        prods = []
        for k in range(NK):
            piece = hs[1, begins[3] + k]
            for v in (2, 1, 0):
                piece = jnp.where(masks[v], hs[1, begins[v] + k], piece)
            prods.append(hs[0, SHIFT + k] * piece)
        put_parts(lx, window11(prods), (0, 128))
        for v in range(SRC):
            prods = [xs[0, SHIFT + k] * xs[v + 1, begins[v] + k] for k in range(NK)]
            put_parts(lhs.at[v // 2], window11(prods), (128 * (v % 2), 256 + 128 * (v % 2)))
        for p in range(SRC // 2):
            total = jnp.dot(lhs[p, :, 0:256], rt[...], preferred_element_type=f32)
            total += jnp.dot(lhs[p, :, 256:512], rt[...], preferred_element_type=f32)
            total += jnp.dot(lx[...], rx3[p], preferred_element_type=f32)
            yy[p] = total
        for i in range(SEG):
            rows = slice(8 * i, 8 * i + 8)
            acc = None
            sub = None
            for v in range(SRC):
                y = yy[v // 2, rows, 128 * (v % 2):128 * (v % 2) + 128]
                a = y * av[v + 1, begins[v] + i]
                s = bv[v + 1, begins[v] + i]
                acc = a if acc is None else acc + a
                sub = s if sub is None else sub + s
            vol[l, i] = av[0, i] * (acc - bv[0, i] * sub)
        return carry

    lax.fori_loop(0, LEVELS, level, 0)

    def pick(i, carry):
        rows = pl.ds(pl.multiple_of(8 * i, 8), 8)
        ht = ht_out[rows, :]
        centre = up[rows, :]
        num = jnp.zeros((8, 128), f32)
        den = jnp.zeros((8, 128), f32)
        for k in range(HYP):
            table = [vol[l, i] for l in range(LEVELS)]
            for bit in range(4):
                odd = (ht & jnp.int32((1 << (4 * k + bit)) - (1 << 32 if 4 * k + bit == 31 else 0))) != 0
                table = [jnp.where(odd, table[t + 1], table[t]) for t in range(0, len(table), 2)]
            sel = 10.0 * table[0] - 10.0
            sel_out[k, rows, :] = sel
            cand = (lax.shift_right_logical(ht, 4 * k) & 15).astype(f32)
            d = cand - centre
            w = jnp.exp(sel - 0.1 * (d * d))
            num += w * cand
            den += w
        red_out[rows, :] = num / den
        return carry

    lax.fori_loop(0, SEG, pick, 0)


def score(ids, xm, xh, hyp, up):
    vmem = pl.BlockSpec(memory_space=pltpu.VMEM)
    n = SEG * 8
    return pl.pallas_call(
        score_kernel,
        out_shape=(
            jax.ShapeDtypeStruct((HYP, n, 128), f32),
            jax.ShapeDtypeStruct((n, 128), jnp.int32),
            jax.ShapeDtypeStruct((n, 128), f32),
        ),
        in_specs=[pl.BlockSpec(memory_space=pltpu.SMEM)] + [vmem] * 4,
        out_specs=(vmem,) * 3,
        scratch_shapes=[
            pltpu.VMEM((SRC + 1, NJ, 8, 128), f32),
            pltpu.VMEM((2, NJ, 8, 128), f32),
            pltpu.VMEM((256, 256), bf16),
            pltpu.VMEM((2, 256, 256), bf16),
            pltpu.VMEM((SRC, 256, 256), bf16),
            pltpu.VMEM((NM * 8 + 8, 768), bf16),
            pltpu.VMEM((NM * 8 + 8, 768), bf16),
            pltpu.VMEM((NM * 8, 256), f32),
            pltpu.VMEM((SRC + 1, NM, 8, 128), f32),
            pltpu.VMEM((SRC + 1, NM, 8, 128), f32),
            pltpu.VMEM((2, n, 512), bf16),
            pltpu.VMEM((n, 256), bf16),
            pltpu.VMEM((2, n, 256), f32),
            pltpu.VMEM((LEVELS, SEG, 8, 128), f32),
            pltpu.VMEM((COLS, ROWS), jnp.int32),
        ],
    )(ids, xm, xh, hyp, up)


def border_lanes(red):
    lane = lax.broadcasted_iota(jnp.int32, (8, 128), 1)
    out = jnp.zeros((8, 128), f32)
    for i in range(SEG):
        v = red[8 * i:8 * i + 8, :]
        out = jnp.where(lane == i, jnp.broadcast_to(v[:, 0:1], (8, 128)), out)
        out = jnp.where(lane == SEG + i, jnp.broadcast_to(v[:, 127:128], (8, 128)), out)
    return out


def black_kernel(sel, ht, red, up, above, below, left, right, out, tmp):
    row_index = lax.axis_index("row")
    col_index = lax.axis_index("col")
    row_count = lax.axis_size("row")
    col_count = lax.axis_size("col")
    lane = lax.broadcasted_iota(jnp.int32, (8, 128), 1)
    seg = lax.broadcasted_iota(jnp.int32, (8, 128), 0)
    row_edge = jnp.where((lane == 0) & (row_index == 0), 1.0, 0.0) + jnp.where(
        (lane == ROWS - 1) & (row_index == row_count - 1), 1.0, 0.0)
    above_v = above[...]
    below_v = below[...]
    for i in range(SEG):
        rows = slice(8 * i, 8 * i + 8)
        r = red[rows, :]
        u = up[rows, :]
        h = ht[rows, :]
        north = jnp.where(lane == 0, jnp.broadcast_to(above_v[:, SEG + i:SEG + i + 1], (8, 128)), pltpu.roll(r, 1, 1))
        south = jnp.where(lane == ROWS - 1, jnp.broadcast_to(below_v[:, i:i + 1], (8, 128)), pltpu.roll(r, ROWS - 1, 1))
        if i == 0:
            west = jnp.concatenate([left[7:8, :], red[8 * SEG - 8:8 * SEG - 1, :]], axis=0)
        else:
            west = red[8 * i - 8:8 * i, :]
        if i == SEG - 1:
            east = jnp.concatenate([red[1:8, :], right[0:1, :]], axis=0)
        else:
            east = red[8 * i + 8:8 * i + 16, :]
        count = 4.0 - row_edge
        if i == 0:
            count = count - jnp.where((seg == 0) & (col_index == 0), 1.0, 0.0)
        if i == SEG - 1:
            count = count - jnp.where((seg == 7) & (col_index == col_count - 1), 1.0, 0.0)
        centre = 0.5 * u + 0.5 * (north + south + west + east) / count
        num = jnp.zeros((8, 128), f32)
        den = jnp.zeros((8, 128), f32)
        for k in range(HYP):
            cand = (lax.shift_right_logical(h, 4 * k) & 15).astype(f32)
            d = cand - centre
            w = jnp.exp(sel[k, rows, :] - 0.1 * (d * d))
            num += w * cand
            den += w
        even = ((lane + i) & 1) == 0
        tmp[pl.ds(i, SEGS, stride=SEG), :] = jnp.where(even, r, num / den)
    out[...] = tmp[...].T


def blacken(sel, ht, red, up, above, below, left, right):
    vmem = pl.BlockSpec(memory_space=pltpu.VMEM)
    return pl.pallas_call(
        black_kernel,
        out_shape=jax.ShapeDtypeStruct((ROWS, COLS), f32),
        in_specs=[vmem] * 8,
        out_specs=vmem,
        scratch_shapes=[pltpu.VMEM((COLS, ROWS), f32)],
    )(sel, ht, red, up, above, below, left, right)


def shifted(array, axis, step):
    size = lax.axis_size(axis)
    pairs = [(i, i + step) for i in range(size) if 0 <= i + step < size]
    return lax.ppermute(array, axis, pairs)


def interp_matrix(fine_pos, coarse_start, coarse_pixel_number, coarse_total):
    numerator = 2 * fine_pos + 1 - UPS
    lower = numerator // (2 * UPS)
    fraction = (numerator - lower * 2 * UPS).astype(f32) / (2.0 * UPS)
    low_index = jnp.clip(lower, 0, coarse_total - 1) - coarse_start
    high_index = jnp.clip(lower + 1, 0, coarse_total - 1) - coarse_start
    columns = jnp.arange(coarse_pixel_number, dtype=jnp.int32)
    low_part = jnp.where(columns[None, :] == low_index[:, None], 1.0 - fraction[:, None], 0.0)
    high_part = jnp.where(columns[None, :] == high_index[:, None], fraction[:, None], 0.0)
    return low_part + high_part


def jacobi_step(line_span, disp, conf):
    col_pad = jnp.pad(line_span[1:-1], ((0, 0), (1, 1)))
    neighbours = line_span[:-2] + line_span[2:] + col_pad[:, :-2] + col_pad[:, 2:]
    return (conf * disp + neighbours) / (conf + 4.0)


def upsample(coarse_disp, coarse_conf):
    row_index = lax.axis_index("row")
    col_index = lax.axis_index("col")
    coarse_tile = ROWS // UPS
    disp = lax.all_gather(coarse_disp, "col", axis=0, tiled=True)
    conf = lax.all_gather(coarse_conf, "col", axis=0, tiled=True)
    height, width = disp.shape
    current = disp
    for _ in range(CITER):
        current = jacobi_step(jnp.pad(current, ((1, 1), (0, 0))), disp, conf)
    spread = jnp.pad(current, ((1, 1), (0, 0)))
    piece = lax.dynamic_slice_in_dim(spread, row_index * coarse_tile, coarse_tile + 2, 0)
    row_mat = interp_matrix(row_index * ROWS + jnp.arange(ROWS, dtype=jnp.int32),
                            row_index * coarse_tile - 1, coarse_tile + 2, height)
    order = jnp.arange(COLS, dtype=jnp.int32)
    order = (order % SEGS) * SEG + order // SEGS
    col_mat = interp_matrix(col_index * COLS + order, 0, width, width)
    high = lax.Precision.HIGHEST
    return jnp.dot(col_mat, jnp.dot(row_mat, piece, precision=high).T, precision=high)


def spread_tiles(reference_image, source_images):
    stacked = jnp.concatenate([reference_image[None], source_images], 0)
    above = shifted(stacked[:, ROWS - R:, :], "row", 1)
    below = shifted(stacked[:, :R, :], "row", -1)
    tall = jnp.concatenate([stacked, above, below], 1)
    west = shifted(tall[:, :, COLS - LEFT:], "col", 1)
    east = shifted(tall[:, :, :8], "col", -1)
    wide = jnp.concatenate([west, tall, east], 2)
    wide = jnp.pad(wide, ((0, 0), (0, 0), (PADL - LEFT, 0)))
    turned = jnp.transpose(wide, (0, 2, 1))
    main = turned[:, :, :ROWS]
    edge = turned[:, :, ROWS:]
    ref = jnp.concatenate([edge[0]] * SRC, 1)
    src = jnp.concatenate([edge[v + 1] for v in range(SRC)], 1)
    edges = jnp.pad(jnp.stack([ref, src]), ((0, 0), (0, 0), (0, 128 - SRC * HL)))
    return main, edges


def on_device(reference_image, source_images, hypotheses, source_ids, coarse_disp, coarse_conf):
    up = upsample(coarse_disp, coarse_conf)
    main, edges = spread_tiles(reference_image, source_images)
    sel, ht, red = score(source_ids, main, edges, hypotheses, up)
    border = border_lanes(red)
    above = shifted(border, "row", 1)
    below = shifted(border, "row", -1)
    left = shifted(red[8 * SEG - 8:], "col", 1)
    right = shifted(red[:8], "col", -1)
    return blacken(sel, ht, red, up, above, below, left, right)


def solution(mesh):
    in_specs = (
        P("row", "col"),
        P(None, "row", "col"),
        P(None, "row", "col"),
        P(),
        P("col", None),
        P("col", None),
    )
    return jax.shard_map(
        on_device, mesh=mesh, in_specs=in_specs, out_specs=P("row", "col"), check_vma=False
    )
```

```python
import functools

import jax
import jax.numpy as jnp
from jax import lax
from jax.experimental import pallas as pl
from jax.experimental.pallas import tpu as pltpu
from jax.sharding import PartitionSpec as P

LEVELS = 16
HYP = 8
SRC = 4
MAXID = 3
WIN = 11
UPS = 8
CITER = 4
R = WIN // 2
AREA = float(WIN * WIN)
FLOOR = 1e-05

ROWS, COLS = 128, 256
SEGS = 8
SEG = COLS // SEGS
SHIFT = MAXID * (LEVELS - 1)
LEFT = SHIFT + R
PADL = 56
CI = 320
NJ = SEG + 2 * R + SHIFT
NK = SEG + 2 * R
NM = SEG + SHIFT
HL = 2 * R
bf16 = jnp.bfloat16
f32 = jnp.float32


def window11(vals):
    n = len(vals)
    count = n - WIN + 1
    suf, pre = {}, {}
    for start in range(0, n, WIN):
        stop = min(start + WIN, n)
        if stop - start == WIN and start < count:
            acc = vals[stop - 1]
            suf[stop - 1] = acc
            for i in range(stop - 2, start - 1, -1):
                acc = vals[i] + acc
                suf[i] = acc
        if start:
            acc = vals[start]
            pre[start] = acc
            for i in range(start + 1, min(stop, start + WIN - 1)):
                acc = acc + vals[i]
                pre[i] = acc
    return [suf[i] if i % WIN == 0 else suf[i] + pre[i + WIN - 1] for i in range(count)]


def parts(value, count):
    out = []
    for _ in range(count - 1):
        piece = value.astype(bf16)
        out.append(piece)
        value = value - piece.astype(f32)
    out.append(value.astype(bf16))
    return out


def put_parts(ref, sums, columns):
    n = len(sums)
    for q in range(0, n, 2):
        both = jnp.concatenate(sums[q:q + 2], axis=0) if q + 1 < n else sums[q]
        for piece, col in zip(parts(both, len(columns)), columns):
            ref[8 * q:8 * q + both.shape[0], col:col + 128] = piece


def band_main():
    a = lax.broadcasted_iota(jnp.int32, (ROWS, ROWS), 0)
    b = lax.broadcasted_iota(jnp.int32, (ROWS, ROWS), 1)
    return jnp.where(jnp.abs(a - b) <= R, 1.0, 0.0).astype(bf16)


def band_halo(view):
    a = lax.broadcasted_iota(jnp.int32, (128, ROWS), 0) - view * HL
    b = lax.broadcasted_iota(jnp.int32, (128, ROWS), 1)
    row = jnp.where(a < R, a - R, a - R + ROWS)
    good = (a >= 0) & (a < HL) & (jnp.abs(row - b) <= R)
    return jnp.where(good, 1.0, 0.0).astype(bf16)


MESH = pl.DeviceIdType.MESH


def exchange_kernel(ref, src, hyp, disp, conf, xm, href, hsrc, cb, ht, htc, send, recv, local):
    row, col = lax.axis_index("row"), lax.axis_index("col")
    nr, nc = lax.axis_size("row"), lax.axis_size("col")
    wide = cb.shape[2]
    last = (disp.shape[1] - wide) // 128

    def inside(dr, dc):
        good = row >= 0
        if dr:
            good = good & ((row > 0) if dr < 0 else (row < nr - 1))
        if dc:
            good = good & ((col > 0) if dc < 0 else (col < nc - 1))
        return good

    def away(dr, dc):
        return {"row": lax.rem(row + dr + nr, nr), "col": lax.rem(col + dc + nc, nc)}

    def tile(j):
        return pl.ds(pl.multiple_of(128 * jnp.clip((32 * j - 32 + 27) // 128, 0, last), 128), wide)

    around = [(dr, dc) for dr in (-1, 0, 1) for dc in (-1, 0, 1) if dr or dc]

    par, home = row // nc, lax.rem(row, nc)
    main_to = {"row": 2 * col + par, "col": home}
    main_from = {"row": nc * lax.rem(row, 2) + col, "col": row // 2}
    own = (2 * col + par == row) & (home == col)
    other = jnp.logical_not(own)
    side_to_row = 2 * col + 2 - 3 * par
    side_sends = (side_to_row >= 0) & (side_to_row < nr)
    side_to = {"row": jnp.clip(side_to_row, 0, nr - 1), "col": home}
    odd = lax.rem(row, 2)
    side_col = row // 2 - 1 + 2 * odd
    side_comes = (side_col >= 0) & (side_col < nc)
    side_from = {"row": nc * odd + col, "col": jnp.clip(side_col, 0, nc - 1)}

    barrier = pltpu.get_barrier_semaphore()
    expected = jnp.int32(0)
    for dr, dc in around:
        expected += inside(dr, dc).astype(jnp.int32)

        @pl.when(inside(dr, dc))
        def _(dr=dr, dc=dc):
            pl.semaphore_signal(barrier, inc=1, device_id=away(dr, dc), device_id_type=MESH)

    @pl.when(other)
    def _():
        pl.semaphore_signal(barrier, inc=1, device_id=main_from, device_id_type=MESH)

    @pl.when(side_comes)
    def _():
        pl.semaphore_signal(barrier, inc=1, device_id=side_from, device_id_type=MESH)

    expected += other.astype(jnp.int32) + side_sends.astype(jnp.int32)
    pl.semaphore_wait(barrier, expected)

    copies = []

    def push(dr, dc, source, target):
        n = len(copies)
        copy = pltpu.make_async_remote_copy(source, target, send.at[n], recv.at[n], device_id=away(dr, dc), device_id_type=MESH)
        copies.append((dr, dc, copy, target))

        @pl.when(inside(dr, dc))
        def _():
            copy.start()

    for dr in (1, -1):
        here = pl.ds(ROWS - 8, 8) if dr == 1 else pl.ds(0, 8)
        side = 0 if dr == 1 else 1
        for dc in (1, -1, 0):
            lanes = {0: (0, COLS), 1: (COLS - 128, 128), -1: (0, 128)}[dc]
            to = {0: 128, 1: 0, -1: 384}[dc]
            push(dr, dc, src.at[:, here, pl.ds(*lanes)], hsrc.at[side, :, :, pl.ds(to, lanes[1])])
            push(dr, dc, ref.at[here, pl.ds(*lanes)], href.at[side, :, pl.ds(to, lanes[1])])

    coarse = []
    for m, array in enumerate((disp, conf)):
        main_src = array.at[pl.ds(pl.multiple_of(8 * par, 8), 24), tile(home)]
        main_dst = cb.at[m, pl.ds(pl.multiple_of(8 - 8 * par, 8), 24), :]
        side_src = array.at[pl.ds(pl.multiple_of(24 - 24 * par, 8), 8), tile(home)]
        side_dst = cb.at[m, pl.ds(pl.multiple_of(24 * par, 8), 8), :]
        n = 20 + 2 * m
        main = pltpu.make_async_remote_copy(main_src, main_dst, send.at[n], recv.at[n], device_id=main_to, device_id_type=MESH)
        mine = pltpu.make_async_copy(main_src, main_dst, local.at[m])
        rest = pltpu.make_async_remote_copy(side_src, side_dst, send.at[n + 1], recv.at[n + 1], device_id=side_to, device_id_type=MESH)
        main_in = cb.at[m, pl.ds(pl.multiple_of(8 - 8 * odd, 8), 24), :]
        side_in = cb.at[m, pl.ds(pl.multiple_of(24 * odd, 8), 8), :]
        got_main = pltpu.make_async_remote_copy(main_src, main_in, send.at[n], recv.at[n], device_id=main_to, device_id_type=MESH)
        got_side = pltpu.make_async_remote_copy(side_src, side_in, send.at[n + 1], recv.at[n + 1], device_id=side_to, device_id_type=MESH)
        coarse.append((main, mine, rest, got_main, got_side, side_in))

        @pl.when(other)
        def _(main=main):
            main.start()

        @pl.when(own)
        def _(mine=mine):
            mine.start()

        @pl.when(side_sends)
        def _(rest=rest):
            rest.start()

    for v in range(SRC):
        xm[v + 1, PADL:PADL + COLS, :] = src[v].T
    xm[0, PADL:PADL + COLS, :] = ref[...].T
    push(0, 1, xm.at[pl.ds(1, SRC), pl.ds(COLS, PADL), :], xm.at[pl.ds(1, SRC), pl.ds(0, PADL), :])
    push(0, 1, xm.at[pl.ds(0, 1), pl.ds(PADL + COLS - 8, 8), :], xm.at[pl.ds(0, 1), pl.ds(PADL - 8, 8), :])
    push(0, -1, xm.at[:, pl.ds(PADL, 8), :], xm.at[:, pl.ds(PADL + COLS, 8), :])

    packed = hyp[0]
    for k in range(1, HYP):
        packed = packed | (hyp[k] << (4 * k))
    htc[...] = packed.T
    for i in range(SEG):
        ht[8 * i:8 * i + 8, :] = htc[pl.ds(i, SEGS, stride=SEG), :]

    for dr, dc, copy, target in copies:
        @pl.when(inside(-dr, -dc))
        def _(copy=copy):
            copy.wait_recv()

        @pl.when(jnp.logical_not(inside(-dr, -dc)))
        def _(target=target):
            target[...] = jnp.zeros(target.shape, f32)

    for main, mine, rest, got_main, got_side, side_in in coarse:
        @pl.when(other)
        def _(got_main=got_main):
            got_main.wait_recv()

        @pl.when(own)
        def _(mine=mine):
            mine.wait()

        @pl.when(side_comes)
        def _(got_side=got_side):
            got_side.wait_recv()

        @pl.when(jnp.logical_not(side_comes))
        def _(side_in=side_in):
            side_in[...] = jnp.zeros(side_in.shape, f32)

        @pl.when(other)
        def _(main=main):
            main.wait_send()

        @pl.when(side_sends)
        def _(rest=rest):
            rest.wait_send()

    for dr, dc, copy, target in copies:
        @pl.when(inside(dr, dc))
        def _(copy=copy):
            copy.wait_send()


def exchange(ref, src, hyp, disp, conf):
    vmem = pl.BlockSpec(memory_space=pltpu.VMEM)
    wide = min(256, disp.shape[1])
    return pl.pallas_call(
        exchange_kernel,
        out_shape=(
            jax.ShapeDtypeStruct((SRC + 1, CI, 128), f32),
            jax.ShapeDtypeStruct((2, 8, 512), f32),
            jax.ShapeDtypeStruct((2, SRC, 8, 512), f32),
            jax.ShapeDtypeStruct((2, 32, wide), f32),
            jax.ShapeDtypeStruct((COLS, 128), jnp.int32),
        ),
        in_specs=[vmem] * 5,
        out_specs=(vmem,) * 5,
        scratch_shapes=[
            pltpu.VMEM((COLS, ROWS), jnp.int32),
            pltpu.SemaphoreType.DMA((24,)),
            pltpu.SemaphoreType.DMA((24,)),
            pltpu.SemaphoreType.DMA((2,)),
        ],
        compiler_params=pltpu.CompilerParams(collective_id=0, has_side_effects=True),
    )(ref, src, hyp, disp, conf)


def interp_block(fine, coarse_start, total, shape):
    numerator = 2 * fine + 1 - UPS
    lower = numerator >> 4
    fraction = (numerator - lower * 2 * UPS).astype(f32) / (2.0 * UPS)
    where = lax.broadcasted_iota(jnp.int32, shape, 1) + coarse_start
    low = jnp.where(where == jnp.clip(lower, 0, total - 1), 1.0 - fraction, 0.0)
    high = jnp.where(where == jnp.clip(lower + 1, 0, total - 1), fraction, 0.0)
    return low + high


def upsampled_tile(cb, total_rows, total_cols):
    row, col = lax.axis_index("row"), lax.axis_index("col")
    high, wide = cb.shape[1:]
    start = 16 * row - 8
    begin = 128 * jnp.clip((32 * col - 32 + 27) // 128, 0, (total_cols - wide) // 128)
    disp, conf = cb[0], cb[1]
    place = lax.broadcasted_iota(jnp.int32, (high, wide), 0) + start
    lane = lax.broadcasted_iota(jnp.int32, (high, wide), 1)
    good = (place >= 0) & (place < total_rows)
    local = lax.broadcasted_iota(jnp.int32, (high, wide), 0)
    pull = conf * disp
    current = disp
    for _ in range(CITER):
        up = jnp.where(local == 0, 0.0, pltpu.roll(current, 1, 0))
        down = jnp.where(local == high - 1, 0.0, pltpu.roll(current, high - 1, 0))
        left = jnp.where(lane == 0, 0.0, pltpu.roll(current, 1, 1))
        right = jnp.where(lane == wide - 1, 0.0, pltpu.roll(current, wide - 1, 1))
        current = jnp.where(good, (pull + (up + down + left + right)) / (conf + 4.0), 0.0)
    fine_rows = row * ROWS + lax.broadcasted_iota(jnp.int32, (ROWS, high), 0)
    order = lax.broadcasted_iota(jnp.int32, (COLS, wide), 0)
    fine_cols = col * COLS + (order & (SEGS - 1)) * SEG + (order >> 3)
    row_mat = interp_block(fine_rows, start, total_rows, (ROWS, high))
    col_mat = interp_block(fine_cols, begin, total_cols, (COLS, wide))
    best = lax.Precision.HIGHEST
    tall = jnp.dot(row_mat, current, precision=best, preferred_element_type=f32)
    return lax.dot_general(col_mat, tall, (((1,), (1,)), ((), ())), precision=best, preferred_element_type=f32)


def score_kernel(coarse_shape, ids, xm, href, hsrc, cb, ht_ref, sel_out, up, red_out, lanes_out,
                 xs, hs, rt, rx3, rmom, xmom, lmom, cmom, av, bv, lhs, lx, yy, vol, zt):
    up[...] = upsampled_tile(cb, *coarse_shape)
    gap = jnp.zeros((64 - SRC * HL, 512), f32)
    stack = []
    for v in range(SRC):
        stack += [hsrc[0, v, 8 - R:8, :], hsrc[1, v, 0:R, :]]
    stack.append(gap)
    for v in range(SRC):
        stack += [href[0, 8 - R:8, :], href[1, 0:R, :]]
    stack.append(gap)
    zt[...] = jnp.concatenate(stack, axis=0).T
    zero = jnp.zeros((128, 128), bf16)
    b = band_main()
    halo = [band_halo(v) for v in range(SRC)]
    rt[0:128, 0:128] = b
    rt[0:128, 128:256] = zero
    rt[128:256, 0:128] = zero
    rt[128:256, 128:256] = b
    for v in range(SRC):
        rmom[v, 0:128, 0:128] = halo[v]
        rmom[v, 0:128, 128:256] = zero
        rmom[v, 128:256, 0:128] = zero
        rmom[v, 128:256, 128:256] = halo[v]
        p, q = v // 2, v % 2
        rx3[p, 0:128, 128 * q:128 * q + 128] = halo[v]
        rx3[p, 128:256, 128 * q:128 * q + 128] = halo[v]

    for j in range(NJ):
        rows = pl.ds(j + PADL - LEFT, SEGS, stride=SEG)
        for v in range(SRC):
            xs[v + 1, j] = xm[v + 1, rows, :]
        edge = zt[pl.ds(j + 128 - LEFT, SEGS, stride=SEG), :]
        hs[1, j] = edge
        if j >= SHIFT:
            xs[0, j] = xm[0, rows, :]
            hs[0, j] = pltpu.roll(edge, 64, 1)

    def moments(load, first, count, ref):
        vals = [load(first + j) for j in range(count)]
        put_parts(ref, window11(vals), (0, 256, 512))
        vals = [load(first + j) for j in range(count)]
        put_parts(ref, window11([x * x for x in vals]), (128, 384, 640))

    def finish(rows, view):
        total = jnp.dot(lmom[0:rows, 0:256], rt[...], preferred_element_type=f32)
        for t in (256, 512):
            total += jnp.dot(lmom[0:rows, t:t + 256], rt[...], preferred_element_type=f32)
        for t in (0, 256, 512):
            total += jnp.dot(xmom[0:rows, t:t + 256], rmom[view], preferred_element_type=f32)
        cmom[0:rows, :] = total

    moments(lambda j: hs[0, j], SHIFT, NK, xmom)
    moments(lambda j: xs[0, j], SHIFT, NK, lmom)
    finish(SEG * 8, 0)
    for i in range(SEG):
        m = cmom[8 * i:8 * i + 8, 0:128] / AREA
        var = cmom[8 * i:8 * i + 8, 128:256] / AREA - m * m + FLOOR
        av[0, i] = lax.rsqrt(var)
        bv[0, i] = m

    moments(lambda j: hs[1, j], 0, NJ, xmom)

    def view_moments(v, carry):
        moments(lambda j: xs[v + 1, j], 0, NJ, lmom)
        finish(NM * 8, v)

        def fill(i, c):
            rows = pl.ds(pl.multiple_of(8 * i, 8), 8)
            m = cmom[rows, 0:128] / AREA
            var = cmom[rows, 128:256] / AREA - m * m + FLOOR
            inv = lax.rsqrt(var) / SRC
            av[v + 1, i] = inv / AREA
            bv[v + 1, i] = m * inv
            return c

        return lax.fori_loop(0, NM, fill, carry)

    lax.fori_loop(0, SRC, view_moments, 0)

    lane = lax.broadcasted_iota(jnp.int32, (8, 128), 1)
    masks = [lane < HL * (v + 1) for v in range(SRC - 1)]

    def level(l, carry):
        begins = [SHIFT - ids[v] * l for v in range(SRC)]
        prods = []
        for k in range(NK):
            piece = hs[1, begins[3] + k]
            for v in (2, 1, 0):
                piece = jnp.where(masks[v], hs[1, begins[v] + k], piece)
            prods.append(hs[0, SHIFT + k] * piece)
        put_parts(lx, window11(prods), (0, 128))
        for v in range(SRC):
            prods = [xs[0, SHIFT + k] * xs[v + 1, begins[v] + k] for k in range(NK)]
            put_parts(lhs.at[v // 2], window11(prods), (128 * (v % 2), 256 + 128 * (v % 2)))
        for p in range(SRC // 2):
            total = jnp.dot(lhs[p, :, 0:256], rt[...], preferred_element_type=f32)
            total += jnp.dot(lhs[p, :, 256:512], rt[...], preferred_element_type=f32)
            total += jnp.dot(lx[...], rx3[p], preferred_element_type=f32)
            yy[p] = total
        for i in range(SEG):
            rows = slice(8 * i, 8 * i + 8)
            acc = None
            sub = None
            for v in range(SRC):
                y = yy[v // 2, rows, 128 * (v % 2):128 * (v % 2) + 128]
                a = y * av[v + 1, begins[v] + i]
                s = bv[v + 1, begins[v] + i]
                acc = a if acc is None else acc + a
                sub = s if sub is None else sub + s
            vol[l, i] = av[0, i] * (acc - bv[0, i] * sub)
        return carry

    lax.fori_loop(0, LEVELS, level, 0)

    def pick(i, carry):
        rows = pl.ds(pl.multiple_of(8 * i, 8), 8)
        ht = ht_ref[rows, :]
        centre = up[rows, :]
        num = jnp.zeros((8, 128), f32)
        den = jnp.zeros((8, 128), f32)
        for k in range(HYP):
            table = [vol[l, i] for l in range(LEVELS)]
            for bit in range(4):
                odd = (ht & jnp.int32((1 << (4 * k + bit)) - (1 << 32 if 4 * k + bit == 31 else 0))) != 0
                table = [jnp.where(odd, table[t + 1], table[t]) for t in range(0, len(table), 2)]
            sel = 10.0 * table[0] - 10.0
            sel_out[k, rows, :] = sel
            cand = (lax.shift_right_logical(ht, 4 * k) & 15).astype(f32)
            d = cand - centre
            w = jnp.exp(sel - 0.1 * (d * d))
            num += w * cand
            den += w
        red_out[rows, :] = num / den
        return carry

    lax.fori_loop(0, SEG, pick, 0)


    lane = lax.broadcasted_iota(jnp.int32, (8, 128), 1)
    border = jnp.zeros((8, 128), f32)
    for i in range(SEG):
        v = red_out[8 * i:8 * i + 8, :]
        border = jnp.where(lane == i, jnp.broadcast_to(v[:, 0:1], (8, 128)), border)
        border = jnp.where(lane == SEG + i, jnp.broadcast_to(v[:, 127:128], (8, 128)), border)
    lanes_out[...] = border


def score(ids, xm, href, hsrc, cb, ht, coarse_shape):
    vmem = pl.BlockSpec(memory_space=pltpu.VMEM)
    n = SEG * 8
    return pl.pallas_call(
        functools.partial(score_kernel, coarse_shape),
        out_shape=(
            jax.ShapeDtypeStruct((HYP, n, 128), f32),
            jax.ShapeDtypeStruct((n, 128), f32),
            jax.ShapeDtypeStruct((n, 128), f32),
            jax.ShapeDtypeStruct((8, 128), f32),
        ),
        in_specs=[pl.BlockSpec(memory_space=pltpu.SMEM)] + [vmem] * 5,
        out_specs=(vmem,) * 4,
        scratch_shapes=[
            pltpu.VMEM((SRC + 1, NJ, 8, 128), f32),
            pltpu.VMEM((2, NJ, 8, 128), f32),
            pltpu.VMEM((256, 256), bf16),
            pltpu.VMEM((2, 256, 256), bf16),
            pltpu.VMEM((SRC, 256, 256), bf16),
            pltpu.VMEM((NM * 8 + 8, 768), bf16),
            pltpu.VMEM((NM * 8 + 8, 768), bf16),
            pltpu.VMEM((NM * 8, 256), f32),
            pltpu.VMEM((SRC + 1, NM, 8, 128), f32),
            pltpu.VMEM((SRC + 1, NM, 8, 128), f32),
            pltpu.VMEM((2, n, 512), bf16),
            pltpu.VMEM((n, 256), bf16),
            pltpu.VMEM((2, n, 256), f32),
            pltpu.VMEM((LEVELS, SEG, 8, 128), f32),
            pltpu.VMEM((512, 128), f32),
        ],
    )(ids, xm, href, hsrc, cb, ht)


def black_kernel(sel, ht, red, up, border, out, tmp, near, send, recv):
    row_index = lax.axis_index("row")
    col_index = lax.axis_index("col")
    row_count = lax.axis_size("row")
    col_count = lax.axis_size("col")
    lane = lax.broadcasted_iota(jnp.int32, (8, 128), 1)
    seg = lax.broadcasted_iota(jnp.int32, (8, 128), 0)
    row_edge = jnp.where((lane == 0) & (row_index == 0), 1.0, 0.0) + jnp.where(
        (lane == ROWS - 1) & (row_index == row_count - 1), 1.0, 0.0)
    def inside(dr, dc):
        if dr:
            return (row_index > 0) if dr < 0 else (row_index < row_count - 1)
        return (col_index > 0) if dc < 0 else (col_index < col_count - 1)

    def away(dr, dc):
        return {"row": lax.rem(row_index + dr + row_count, row_count),
                "col": lax.rem(col_index + dc + col_count, col_count)}

    around = [(1, 0), (-1, 0), (0, 1), (0, -1)]
    sources = [border, border, red.at[pl.ds(8 * SEG - 8, 8), :], red.at[pl.ds(0, 8), :]]
    barrier = pltpu.get_barrier_semaphore()
    expected = jnp.int32(0)
    for dr, dc in around:
        expected += inside(dr, dc).astype(jnp.int32)

        @pl.when(inside(dr, dc))
        def _(dr=dr, dc=dc):
            pl.semaphore_signal(barrier, inc=1, device_id=away(dr, dc), device_id_type=MESH)

    pl.semaphore_wait(barrier, expected)
    copies = []
    for n, (dr, dc) in enumerate(around):
        copy = pltpu.make_async_remote_copy(sources[n], near.at[n], send.at[n], recv.at[n], device_id=away(dr, dc), device_id_type=MESH)
        copies.append(copy)

        @pl.when(inside(dr, dc))
        def _(copy=copy):
            copy.start()

    for n, (dr, dc) in enumerate(around):
        @pl.when(inside(-dr, -dc))
        def _(n=n):
            copies[n].wait_recv()

        @pl.when(jnp.logical_not(inside(-dr, -dc)))
        def _(n=n):
            near[n] = jnp.zeros((8, 128), f32)

        @pl.when(inside(dr, dc))
        def _(n=n):
            copies[n].wait_send()

    above_v = near[0]
    below_v = near[1]
    left, right = near.at[2], near.at[3]
    for i in range(SEG):
        rows = slice(8 * i, 8 * i + 8)
        r = red[rows, :]
        u = up[rows, :]
        h = ht[rows, :]
        north = jnp.where(lane == 0, jnp.broadcast_to(above_v[:, SEG + i:SEG + i + 1], (8, 128)), pltpu.roll(r, 1, 1))
        south = jnp.where(lane == ROWS - 1, jnp.broadcast_to(below_v[:, i:i + 1], (8, 128)), pltpu.roll(r, ROWS - 1, 1))
        if i == 0:
            west = jnp.concatenate([left[7:8, :], red[8 * SEG - 8:8 * SEG - 1, :]], axis=0)
        else:
            west = red[8 * i - 8:8 * i, :]
        if i == SEG - 1:
            east = jnp.concatenate([red[1:8, :], right[0:1, :]], axis=0)
        else:
            east = red[8 * i + 8:8 * i + 16, :]
        count = 4.0 - row_edge
        if i == 0:
            count = count - jnp.where((seg == 0) & (col_index == 0), 1.0, 0.0)
        if i == SEG - 1:
            count = count - jnp.where((seg == 7) & (col_index == col_count - 1), 1.0, 0.0)
        centre = 0.5 * u + 0.5 * (north + south + west + east) / count
        num = jnp.zeros((8, 128), f32)
        den = jnp.zeros((8, 128), f32)
        for k in range(HYP):
            cand = (lax.shift_right_logical(h, 4 * k) & 15).astype(f32)
            d = cand - centre
            w = jnp.exp(sel[k, rows, :] - 0.1 * (d * d))
            num += w * cand
            den += w
        even = ((lane + i) & 1) == 0
        tmp[pl.ds(i, SEGS, stride=SEG), :] = jnp.where(even, r, num / den)
    out[...] = tmp[...].T


def blacken(sel, ht, red, up, border):
    vmem = pl.BlockSpec(memory_space=pltpu.VMEM)
    return pl.pallas_call(
        black_kernel,
        out_shape=jax.ShapeDtypeStruct((ROWS, COLS), f32),
        in_specs=[vmem] * 5,
        out_specs=vmem,
        scratch_shapes=[
            pltpu.VMEM((COLS, ROWS), f32),
            pltpu.VMEM((4, 8, 128), f32),
            pltpu.SemaphoreType.DMA((4,)),
            pltpu.SemaphoreType.DMA((4,)),
        ],
        compiler_params=pltpu.CompilerParams(collective_id=1, has_side_effects=True),
    )(sel, ht, red, up, border)


def on_device(reference_image, source_images, hypotheses, source_ids, coarse_disp, coarse_conf):
    xm, href, hsrc, cb, ht = exchange(reference_image, source_images, hypotheses, coarse_disp, coarse_conf)
    shape = (coarse_disp.shape[0] * lax.axis_size("col"), coarse_disp.shape[1])
    sel, up, red, border = score(source_ids, xm, href, hsrc, cb, ht, shape)
    return blacken(sel, ht, red, up, border)


def solution(mesh):
    in_specs = (
        P("row", "col"),
        P(None, "row", "col"),
        P(None, "row", "col"),
        P(),
        P("col", None),
        P("col", None),
    )
    return jax.shard_map(
        on_device, mesh=mesh, in_specs=in_specs, out_specs=P("row", "col"), check_vma=False
    )
```

```python
import functools

import jax
import jax.numpy as jnp
from jax import lax
from jax.experimental import pallas as pl
from jax.experimental.pallas import tpu as pltpu
from jax.sharding import PartitionSpec as P

LEVELS = 16
HYP = 8
SRC = 4
MAXID = 3
WIN = 11
UPS = 8
CITER = 4
R = WIN // 2
AREA = float(WIN * WIN)
FLOOR = 1e-05

ROWS, COLS = 128, 256
SEGS = 8
SEG = COLS // SEGS
SHIFT = MAXID * (LEVELS - 1)
LEFT = SHIFT + R
PADL = 56
CI = 320
NJ = SEG + 2 * R + SHIFT
NK = SEG + 2 * R
NM = SEG + SHIFT
HL = 2 * R
bf16 = jnp.bfloat16
f32 = jnp.float32


def window11(vals):
    n = len(vals)
    count = n - WIN + 1
    suf, pre = {}, {}
    for start in range(0, n, WIN):
        stop = min(start + WIN, n)
        if stop - start == WIN and start < count:
            acc = vals[stop - 1]
            suf[stop - 1] = acc
            for i in range(stop - 2, start - 1, -1):
                acc = vals[i] + acc
                suf[i] = acc
        if start:
            acc = vals[start]
            pre[start] = acc
            for i in range(start + 1, min(stop, start + WIN - 1)):
                acc = acc + vals[i]
                pre[i] = acc
    return [suf[i] if i % WIN == 0 else suf[i] + pre[i + WIN - 1] for i in range(count)]


def parts(value, count):
    out = []
    for _ in range(count - 1):
        piece = value.astype(bf16)
        out.append(piece)
        value = value - piece.astype(f32)
    out.append(value.astype(bf16))
    return out


def put_parts(ref, sums, columns):
    n = len(sums)
    for q in range(0, n, 2):
        both = jnp.concatenate(sums[q:q + 2], axis=0) if q + 1 < n else sums[q]
        for piece, col in zip(parts(both, len(columns)), columns):
            ref[8 * q:8 * q + both.shape[0], col:col + 128] = piece


def band_main():
    a = lax.broadcasted_iota(jnp.int32, (ROWS, ROWS), 0)
    b = lax.broadcasted_iota(jnp.int32, (ROWS, ROWS), 1)
    return jnp.where(jnp.abs(a - b) <= R, 1.0, 0.0).astype(bf16)


def band_halo(view):
    a = lax.broadcasted_iota(jnp.int32, (128, ROWS), 0) - view * HL
    b = lax.broadcasted_iota(jnp.int32, (128, ROWS), 1)
    row = jnp.where(a < R, a - R, a - R + ROWS)
    good = (a >= 0) & (a < HL) & (jnp.abs(row - b) <= R)
    return jnp.where(good, 1.0, 0.0).astype(bf16)


def interp_block(fine, coarse_start, total, shape):
    numerator = 2 * fine + 1 - UPS
    lower = numerator >> 4
    fraction = (numerator - lower * 2 * UPS).astype(f32) / (2.0 * UPS)
    where = lax.broadcasted_iota(jnp.int32, shape, 1) + coarse_start
    low = jnp.where(where == jnp.clip(lower, 0, total - 1), 1.0 - fraction, 0.0)
    high = jnp.where(where == jnp.clip(lower + 1, 0, total - 1), fraction, 0.0)
    return low + high


def upsampled_tile(cb, total_rows, total_cols):
    row, col = lax.axis_index("row"), lax.axis_index("col")
    high, wide = cb.shape[1:]
    start = 16 * row - 8
    begin = 128 * jnp.clip((32 * col + 123) // 128 - 1, 0, (total_cols - wide) // 128)
    disp, conf = cb[0], cb[1]
    place = lax.broadcasted_iota(jnp.int32, (high, wide), 0) + start
    lane = lax.broadcasted_iota(jnp.int32, (high, wide), 1)
    good = (place >= 0) & (place < total_rows)
    local = lax.broadcasted_iota(jnp.int32, (high, wide), 0)
    pull = conf * disp
    current = disp
    for _ in range(CITER):
        up = jnp.where(local == 0, 0.0, pltpu.roll(current, 1, 0))
        down = jnp.where(local == high - 1, 0.0, pltpu.roll(current, high - 1, 0))
        left = jnp.where(lane == 0, 0.0, pltpu.roll(current, 1, 1))
        right = jnp.where(lane == wide - 1, 0.0, pltpu.roll(current, wide - 1, 1))
        current = jnp.where(good, (pull + (up + down + left + right)) / (conf + 4.0), 0.0)
    fine_rows = row * ROWS + lax.broadcasted_iota(jnp.int32, (ROWS, high), 0)
    order = lax.broadcasted_iota(jnp.int32, (COLS, wide), 0)
    fine_cols = col * COLS + (order & (SEGS - 1)) * SEG + (order >> 3)
    row_mat = interp_block(fine_rows, start, total_rows, (ROWS, high))
    col_mat = interp_block(fine_cols, begin, total_cols, (COLS, wide))
    best = lax.Precision.HIGHEST
    tall = jnp.dot(row_mat, current, precision=best, preferred_element_type=f32)
    return lax.dot_general(col_mat, tall, (((1,), (1,)), ((), ())), precision=best, preferred_element_type=f32)


MESH = pl.DeviceIdType.MESH


def stereo_kernel(coarse_shape, ids, ref_in, src_in, hyp_in, disp_in, conf_in, out,
                  img, hyp, coarse, xm, hal, cb, ht, htc, sel, up, red, border, tmp, near,
                  xs, hs, rt, rx3, rmom, xmom, lmom, cmom, av, bv, lhs, lx, yy, vol, zt,
                  load, local, send, recv, csend, crecv):
    row, col = lax.axis_index("row"), lax.axis_index("col")
    nr, nc = lax.axis_size("row"), lax.axis_size("col")
    wide = cb.shape[2]
    last = (coarse_shape[1] - wide) // 128

    loads = [
        pltpu.make_async_copy(ref_in, img.at[0], load.at[0]),
        pltpu.make_async_copy(src_in, img.at[pl.ds(1, SRC)], load.at[1]),
        pltpu.make_async_copy(disp_in, coarse.at[0], load.at[2]),
        pltpu.make_async_copy(conf_in, coarse.at[1], load.at[3]),
        pltpu.make_async_copy(hyp_in, hyp, load.at[4]),
    ]
    for copy in loads:
        copy.start()

    def inside(dr, dc):
        good = row >= 0
        if dr:
            good = good & ((row > 0) if dr < 0 else (row < nr - 1))
        if dc:
            good = good & ((col > 0) if dc < 0 else (col < nc - 1))
        return good

    def away(dr, dc):
        return {"row": lax.rem(row + dr + nr, nr), "col": lax.rem(col + dc + nc, nc)}

    around = [(dr, dc) for dr in (-1, 0, 1) for dc in (-1, 0, 1) if dr or dc]
    odd = lax.rem(row, 2)
    main_col = row // 2
    side_col = main_col - 1 + 2 * odd
    side_there = (side_col >= 0) & (side_col < nc)
    is_main = col == main_col
    is_side = col == side_col

    barrier = pltpu.get_barrier_semaphore()
    expected = jnp.int32(0)
    for dr, dc in around:
        expected += inside(dr, dc).astype(jnp.int32)

        @pl.when(inside(dr, dc))
        def _(dr=dr, dc=dc):
            pl.semaphore_signal(barrier, inc=1, device_id=away(dr, dc), device_id_type=MESH)

    @pl.when(jnp.logical_not(is_main))
    def _():
        pl.semaphore_signal(barrier, inc=1, device_id={"row": row, "col": main_col}, device_id_type=MESH)

    @pl.when(side_there & jnp.logical_not(is_side))
    def _():
        pl.semaphore_signal(barrier, inc=1, device_id={"row": row, "col": jnp.clip(side_col, 0, nc - 1)}, device_id_type=MESH)

    expected += (nc - 1) * (is_main.astype(jnp.int32) + is_side.astype(jnp.int32))
    pl.semaphore_wait(barrier, expected)

    copies = []

    def push(dr, dc, source, target):
        n = len(copies)
        copy = pltpu.make_async_remote_copy(source, target, send.at[n], recv.at[n], device_id=away(dr, dc), device_id_type=MESH)
        copies.append((dr, dc, copy, target))

        @pl.when(inside(dr, dc))
        def _():
            copy.start()

    def arrive(entries):
        for dr, dc, copy, target in entries:
            @pl.when(inside(-dr, -dc))
            def _(copy=copy):
                copy.wait_recv()

            @pl.when(jnp.logical_not(inside(-dr, -dc)))
            def _(target=target):
                target[...] = jnp.zeros(target.shape, f32)

    def leave(entries):
        for dr, dc, copy, target in entries:
            @pl.when(inside(dr, dc))
            def _(copy=copy):
                copy.wait_send()

    loads[0].wait()
    loads[1].wait()
    for dc in (1, -1, 0):
        lanes = {0: (0, COLS), 1: (COLS - 128, 128), -1: (0, 128)}[dc]
        to = {0: 128, 1: 0, -1: 384}[dc]
        for dr in (1, -1):
            here = pl.ds(ROWS - 8, 8) if dr == 1 else pl.ds(0, 8)
            side = 0 if dr == 1 else 1
            push(dr, dc, img.at[:, here, pl.ds(*lanes)], hal.at[side, :, :, pl.ds(to, lanes[1])])

    for v in range(SRC + 1):
        xm[v, PADL:PADL + COLS, :] = img[v].T
    push(0, 1, xm.at[pl.ds(1, SRC), pl.ds(COLS, PADL), :], xm.at[pl.ds(1, SRC), pl.ds(0, PADL), :])
    push(0, -1, xm.at[:, pl.ds(PADL, 8), :], xm.at[:, pl.ds(PADL + COLS, 8), :])
    push(0, 1, xm.at[pl.ds(0, 1), pl.ds(PADL + COLS - 8, 8), :], xm.at[pl.ds(0, 1), pl.ds(PADL - 8, 8), :])
    halos = list(copies)

    loads[2].wait()
    loads[3].wait()
    main_src = pl.ds(pl.multiple_of(8 * odd, 8), 24)
    main_dst = cb.at[:, pl.ds(pl.multiple_of(8 - 8 * odd, 8), 24), :]
    side_src = pl.ds(pl.multiple_of(24 - 24 * odd, 8), 8)
    side_dst = cb.at[:, pl.ds(pl.multiple_of(24 * odd, 8), 8), :]

    def coarse_copy(j, rows, target, kind):
        lanes = pl.ds(pl.multiple_of(128 * jnp.clip((32 * j + 123) // 128 - 1, 0, last), 128), wide)
        source = coarse.at[:, rows, lanes]
        return pltpu.make_async_remote_copy(source, target, csend.at[j], crecv.at[kind], device_id={"row": row, "col": j}, device_id_type=MESH)

    def coarse_own(rows, target):
        lanes = pl.ds(pl.multiple_of(128 * jnp.clip((32 * col + 123) // 128 - 1, 0, last), 128), wide)
        return pltpu.make_async_copy(coarse.at[:, rows, lanes], target, local.at[0])

    kinds = ((is_main, main_src, main_dst, 0), (is_side, side_src, side_dst, 1))
    for role, rows, target, kind in kinds:
        @pl.when(role)
        def _(rows=rows, target=target, kind=kind):
            def one(j, carry):
                @pl.when(j != col)
                def _():
                    coarse_copy(j, rows, target, kind).start()

                return carry

            lax.fori_loop(0, nc, one, 0)
            coarse_own(rows, target).start()

    loads[4].wait()
    packed = hyp[0]
    for k in range(1, HYP):
        packed = packed | (hyp[k] << (4 * k))
    htc[...] = packed.T
    for i in range(SEG):
        ht[8 * i:8 * i + 8, :] = htc[pl.ds(i, SEGS, stride=SEG), :]

    zero = jnp.zeros((128, 128), bf16)
    b = band_main()
    halo = [band_halo(v) for v in range(SRC)]
    rt[0:128, 0:128] = b
    rt[0:128, 128:256] = zero
    rt[128:256, 0:128] = zero
    rt[128:256, 128:256] = b
    for v in range(SRC):
        rmom[v, 0:128, 0:128] = halo[v]
        rmom[v, 0:128, 128:256] = zero
        rmom[v, 128:256, 0:128] = zero
        rmom[v, 128:256, 128:256] = halo[v]
        p, q = v // 2, v % 2
        rx3[p, 0:128, 128 * q:128 * q + 128] = halo[v]
        rx3[p, 128:256, 128 * q:128 * q + 128] = halo[v]


    arrive(halos)
    gap = jnp.zeros((64 - SRC * HL, 512), f32)
    stack = []
    for v in range(SRC):
        stack += [hal[0, v + 1, 8 - R:8, :], hal[1, v + 1, 0:R, :]]
    stack.append(gap)
    for v in range(SRC):
        stack += [hal[0, 0, 8 - R:8, :], hal[1, 0, 0:R, :]]
    stack.append(gap)
    zt[...] = jnp.concatenate(stack, axis=0).T
    for j in range(NJ):
        rows = pl.ds(j + PADL - LEFT, SEGS, stride=SEG)
        for v in range(SRC):
            xs[v + 1, j] = xm[v + 1, rows, :]
        edge = zt[pl.ds(j + 128 - LEFT, SEGS, stride=SEG), :]
        hs[1, j] = edge
        if j >= SHIFT:
            xs[0, j] = xm[0, rows, :]
            hs[0, j] = pltpu.roll(edge, 64, 1)

    def moments(load, first, count, ref):
        vals = [load(first + j) for j in range(count)]
        put_parts(ref, window11(vals), (0, 256, 512))
        vals = [load(first + j) for j in range(count)]
        put_parts(ref, window11([x * x for x in vals]), (128, 384, 640))

    def finish(rows, view):
        total = jnp.dot(lmom[0:rows, 0:256], rt[...], preferred_element_type=f32)
        for t in (256, 512):
            total += jnp.dot(lmom[0:rows, t:t + 256], rt[...], preferred_element_type=f32)
        for t in (0, 256, 512):
            total += jnp.dot(xmom[0:rows, t:t + 256], rmom[view], preferred_element_type=f32)
        cmom[0:rows, :] = total

    moments(lambda j: hs[0, j], SHIFT, NK, xmom)
    moments(lambda j: xs[0, j], SHIFT, NK, lmom)
    finish(SEG * 8, 0)
    for i in range(SEG):
        m = cmom[8 * i:8 * i + 8, 0:128] / AREA
        var = cmom[8 * i:8 * i + 8, 128:256] / AREA - m * m + FLOOR
        av[0, i] = lax.rsqrt(var)
        bv[0, i] = m

    moments(lambda j: hs[1, j], 0, NJ, xmom)

    def view_moments(v, carry):
        moments(lambda j: xs[v + 1, j], 0, NJ, lmom)
        finish(NM * 8, v)

        def fill(i, c):
            rows = pl.ds(pl.multiple_of(8 * i, 8), 8)
            m = cmom[rows, 0:128] / AREA
            var = cmom[rows, 128:256] / AREA - m * m + FLOOR
            inv = lax.rsqrt(var) / SRC
            av[v + 1, i] = inv / AREA
            bv[v + 1, i] = m * inv
            return c

        return lax.fori_loop(0, NM, fill, carry)

    lax.fori_loop(0, SRC, view_moments, 0)

    lane = lax.broadcasted_iota(jnp.int32, (8, 128), 1)
    masks = [lane < HL * (v + 1) for v in range(SRC - 1)]

    def level(l, carry):
        begins = [SHIFT - ids[v] * l for v in range(SRC)]
        prods = []
        for k in range(NK):
            piece = hs[1, begins[3] + k]
            for v in (2, 1, 0):
                piece = jnp.where(masks[v], hs[1, begins[v] + k], piece)
            prods.append(hs[0, SHIFT + k] * piece)
        put_parts(lx, window11(prods), (0, 128))
        for v in range(SRC):
            prods = [xs[0, SHIFT + k] * xs[v + 1, begins[v] + k] for k in range(NK)]
            put_parts(lhs.at[v // 2], window11(prods), (128 * (v % 2), 256 + 128 * (v % 2)))
        for p in range(SRC // 2):
            total = jnp.dot(lhs[p, :, 0:256], rt[...], preferred_element_type=f32)
            total += jnp.dot(lhs[p, :, 256:512], rt[...], preferred_element_type=f32)
            total += jnp.dot(lx[...], rx3[p], preferred_element_type=f32)
            yy[p] = total
        for i in range(SEG):
            rows = slice(8 * i, 8 * i + 8)
            acc = None
            sub = None
            for v in range(SRC):
                y = yy[v // 2, rows, 128 * (v % 2):128 * (v % 2) + 128]
                a = y * av[v + 1, begins[v] + i]
                s = bv[v + 1, begins[v] + i]
                acc = a if acc is None else acc + a
                sub = s if sub is None else sub + s
            vol[l, i] = av[0, i] * (acc - bv[0, i] * sub)
        return carry

    lax.fori_loop(0, LEVELS, level, 0)

    for role, rows, target, kind in kinds:
        there = side_there if kind else col >= 0

        @pl.when(role)
        def _(rows=rows, target=target, kind=kind):
            coarse_own(rows, target).wait()

        @pl.when(jnp.logical_not(role) & there)
        def _(rows=rows, target=target, kind=kind):
            coarse_copy(col, rows, target, kind).wait_recv()

    @pl.when(jnp.logical_not(side_there))
    def _():
        side_dst[...] = jnp.zeros(side_dst.shape, f32)

    up[...] = upsampled_tile(cb, *coarse_shape)

    def pick(i, carry):
        rows = pl.ds(pl.multiple_of(8 * i, 8), 8)
        codes = ht[rows, :]
        centre = up[rows, :]
        num = jnp.zeros((8, 128), f32)
        den = jnp.zeros((8, 128), f32)
        for k in range(HYP):
            table = [vol[l, i] for l in range(LEVELS)]
            for bit in range(4):
                odd = (codes & jnp.int32((1 << (4 * k + bit)) - (1 << 32 if 4 * k + bit == 31 else 0))) != 0
                table = [jnp.where(odd, table[t + 1], table[t]) for t in range(0, len(table), 2)]
            gain = 10.0 * table[0] - 10.0
            sel[k, rows, :] = gain
            cand = (lax.shift_right_logical(codes, 4 * k) & 15).astype(f32)
            d = cand - centre
            w = jnp.exp(gain - 0.1 * (d * d))
            num += w * cand
            den += w
        red[rows, :] = num / den
        return carry

    lax.fori_loop(0, SEG, pick, 0)


    lane = lax.broadcasted_iota(jnp.int32, (8, 128), 1)
    edge = jnp.zeros((8, 128), f32)
    for i in range(SEG):
        v = red[8 * i:8 * i + 8, :]
        edge = jnp.where(lane == i, jnp.broadcast_to(v[:, 0:1], (8, 128)), edge)
        edge = jnp.where(lane == SEG + i, jnp.broadcast_to(v[:, 127:128], (8, 128)), edge)
    border[...] = edge


    copies.clear()
    copies.extend(halos)
    push(0, 1, red.at[pl.ds(8 * SEG - 8, 8), :], near.at[2])
    push(0, -1, red.at[pl.ds(0, 8), :], near.at[3])
    push(1, 0, border, near.at[0])
    push(-1, 0, border, near.at[1])
    final = copies[len(halos):]

    leave(halos)
    for role, rows, target, kind in kinds:
        @pl.when(role)
        def _(rows=rows, target=target, kind=kind):
            def one(j, carry):
                @pl.when(j != col)
                def _():
                    coarse_copy(j, rows, target, kind).wait_send()

                return carry

            lax.fori_loop(0, nc, one, 0)

    arrive(final)
    lane = lax.broadcasted_iota(jnp.int32, (8, 128), 1)
    seg = lax.broadcasted_iota(jnp.int32, (8, 128), 0)
    row_edge = jnp.where((lane == 0) & (row == 0), 1.0, 0.0) + jnp.where(
        (lane == ROWS - 1) & (row == nr - 1), 1.0, 0.0)
    above_v = near[0]
    below_v = near[1]
    left, right = near.at[2], near.at[3]
    for i in range(SEG):
        rows = slice(8 * i, 8 * i + 8)
        r = red[rows, :]
        u = up[rows, :]
        h = ht[rows, :]
        north = jnp.where(lane == 0, jnp.broadcast_to(above_v[:, SEG + i:SEG + i + 1], (8, 128)), pltpu.roll(r, 1, 1))
        south = jnp.where(lane == ROWS - 1, jnp.broadcast_to(below_v[:, i:i + 1], (8, 128)), pltpu.roll(r, ROWS - 1, 1))
        if i == 0:
            west = jnp.concatenate([left[7:8, :], red[8 * SEG - 8:8 * SEG - 1, :]], axis=0)
        else:
            west = red[8 * i - 8:8 * i, :]
        if i == SEG - 1:
            east = jnp.concatenate([red[1:8, :], right[0:1, :]], axis=0)
        else:
            east = red[8 * i + 8:8 * i + 16, :]
        count = 4.0 - row_edge
        if i == 0:
            count = count - jnp.where((seg == 0) & (col == 0), 1.0, 0.0)
        if i == SEG - 1:
            count = count - jnp.where((seg == 7) & (col == nc - 1), 1.0, 0.0)
        centre = 0.5 * u + 0.5 * (north + south + west + east) / count
        num = jnp.zeros((8, 128), f32)
        den = jnp.zeros((8, 128), f32)
        for k in range(HYP):
            cand = (lax.shift_right_logical(h, 4 * k) & 15).astype(f32)
            d = cand - centre
            w = jnp.exp(sel[k, rows, :] - 0.1 * (d * d))
            num += w * cand
            den += w
        even = ((lane + i) & 1) == 0
        tmp[pl.ds(i, SEGS, stride=SEG), :] = jnp.where(even, r, num / den)
    out[...] = tmp[...].T
    leave(final)


def on_device(reference_image, source_images, hypotheses, source_ids, coarse_disp, coarse_conf):
    shape = (coarse_disp.shape[0] * lax.axis_size("col"), coarse_disp.shape[1])
    anywhere = pl.BlockSpec(memory_space=pl.ANY)
    n = SEG * 8
    return pl.pallas_call(
        functools.partial(stereo_kernel, shape),
        out_shape=jax.ShapeDtypeStruct((ROWS, COLS), f32),
        in_specs=[pl.BlockSpec(memory_space=pltpu.SMEM)] + [anywhere] * 5,
        out_specs=pl.BlockSpec(memory_space=pltpu.VMEM),
        scratch_shapes=[
            pltpu.VMEM((SRC + 1, ROWS, COLS), f32),
            pltpu.VMEM((HYP, ROWS, COLS), jnp.int32),
            pltpu.VMEM((2,) + coarse_disp.shape, f32),
            pltpu.VMEM((SRC + 1, CI, 128), f32),
            pltpu.VMEM((2, SRC + 1, 8, 512), f32),
            pltpu.VMEM((2, 32, min(256, coarse_disp.shape[1])), f32),
            pltpu.VMEM((n, 128), jnp.int32),
            pltpu.VMEM((COLS, ROWS), jnp.int32),
            pltpu.VMEM((HYP, n, 128), f32),
            pltpu.VMEM((n, 128), f32),
            pltpu.VMEM((n, 128), f32),
            pltpu.VMEM((8, 128), f32),
            pltpu.VMEM((COLS, ROWS), f32),
            pltpu.VMEM((4, 8, 128), f32),
            pltpu.VMEM((SRC + 1, NJ, 8, 128), f32),
            pltpu.VMEM((2, NJ, 8, 128), f32),
            pltpu.VMEM((256, 256), bf16),
            pltpu.VMEM((2, 256, 256), bf16),
            pltpu.VMEM((SRC, 256, 256), bf16),
            pltpu.VMEM((NM * 8 + 8, 768), bf16),
            pltpu.VMEM((NM * 8 + 8, 768), bf16),
            pltpu.VMEM((NM * 8, 256), f32),
            pltpu.VMEM((SRC + 1, NM, 8, 128), f32),
            pltpu.VMEM((SRC + 1, NM, 8, 128), f32),
            pltpu.VMEM((2, n, 512), bf16),
            pltpu.VMEM((n, 256), bf16),
            pltpu.VMEM((2, n, 256), f32),
            pltpu.VMEM((LEVELS, SEG, 8, 128), f32),
            pltpu.VMEM((512, 128), f32),
            pltpu.SemaphoreType.DMA((5,)),
            pltpu.SemaphoreType.DMA((1,)),
            pltpu.SemaphoreType.DMA((13,)),
            pltpu.SemaphoreType.DMA((13,)),
            pltpu.SemaphoreType.DMA((16,)),
            pltpu.SemaphoreType.DMA((2,)),
        ],
        compiler_params=pltpu.CompilerParams(collective_id=0, has_side_effects=True),
    )(source_ids, reference_image, source_images, hypotheses, coarse_disp, coarse_conf)


def solution(mesh):
    in_specs = (
        P("row", "col"),
        P(None, "row", "col"),
        P(None, "row", "col"),
        P(),
        P("col", None),
        P("col", None),
    )
    return jax.shard_map(
        on_device, mesh=mesh, in_specs=in_specs, out_specs=P("row", "col"), check_vma=False
    )
```

```python
import functools

import jax
import jax.numpy as jnp
from jax import lax
from jax.experimental import pallas as pl
from jax.experimental.pallas import tpu as pltpu
from jax.sharding import PartitionSpec as P

LEVELS = 16
HYP = 8
SRC = 4
MAXID = 3
WIN = 11
UPS = 8
CITER = 4
R = WIN // 2
AREA = float(WIN * WIN)
FLOOR = 1e-05

ROWS, COLS = 128, 256
SEGS = 8
SEG = COLS // SEGS
SHIFT = MAXID * (LEVELS - 1)
LEFT = SHIFT + R
PADL = 56
CI = 320
NJ = SEG + 2 * R + SHIFT
NK = SEG + 2 * R
NM = SEG + SHIFT
HL = 2 * R
LB = 2
VMEM_LIMIT = 60 * 1024 * 1024
bf16 = jnp.bfloat16
f32 = jnp.float32


def window11(vals):
    n = len(vals)
    count = n - WIN + 1
    suf, pre = {}, {}
    for start in range(0, n, WIN):
        stop = min(start + WIN, n)
        if stop - start == WIN and start < count:
            acc = vals[stop - 1]
            suf[stop - 1] = acc
            for i in range(stop - 2, start - 1, -1):
                acc = vals[i] + acc
                suf[i] = acc
        if start:
            acc = vals[start]
            pre[start] = acc
            for i in range(start + 1, min(stop, start + WIN - 1)):
                acc = acc + vals[i]
                pre[i] = acc
    return [suf[i] if i % WIN == 0 else suf[i] + pre[i + WIN - 1] for i in range(count)]


def parts(value, count):
    out = []
    for _ in range(count - 1):
        piece = value.astype(bf16)
        out.append(piece)
        value = value - piece.astype(f32)
    out.append(value.astype(bf16))
    return out


def put_parts(ref, sums, columns):
    n = len(sums)
    for q in range(0, n, 2):
        both = jnp.concatenate(sums[q:q + 2], axis=0) if q + 1 < n else sums[q]
        for piece, col in zip(parts(both, len(columns)), columns):
            ref[8 * q:8 * q + both.shape[0], col:col + 128] = piece


def band_main():
    a = lax.broadcasted_iota(jnp.int32, (ROWS, ROWS), 0)
    b = lax.broadcasted_iota(jnp.int32, (ROWS, ROWS), 1)
    return jnp.where(jnp.abs(a - b) <= R, 1.0, 0.0).astype(bf16)


def band_halo(view):
    a = lax.broadcasted_iota(jnp.int32, (128, ROWS), 0) - view * HL
    b = lax.broadcasted_iota(jnp.int32, (128, ROWS), 1)
    row = jnp.where(a < R, a - R, a - R + ROWS)
    good = (a >= 0) & (a < HL) & (jnp.abs(row - b) <= R)
    return jnp.where(good, 1.0, 0.0).astype(bf16)


def interp_block(fine, coarse_start, total, shape):
    numerator = 2 * fine + 1 - UPS
    lower = numerator >> 4
    fraction = (numerator - lower * 2 * UPS).astype(f32) / (2.0 * UPS)
    where = lax.broadcasted_iota(jnp.int32, shape, 1) + coarse_start
    low = jnp.where(where == jnp.clip(lower, 0, total - 1), 1.0 - fraction, 0.0)
    high = jnp.where(where == jnp.clip(lower + 1, 0, total - 1), fraction, 0.0)
    return low + high


def coarse_window(total_cols, wide):
    row, col = lax.axis_index("row"), lax.axis_index("col")
    return 16 * row - 8, 128 * jnp.clip((32 * col + 123) // 128 - 1, 0, (total_cols - wide) // 128)


def interp_mats(row_mat, col_mat, total_rows, total_cols):
    row, col = lax.axis_index("row"), lax.axis_index("col")
    high, wide = row_mat.shape[1], col_mat.shape[1]
    start, begin = coarse_window(total_cols, wide)
    fine_rows = row * ROWS + lax.broadcasted_iota(jnp.int32, (ROWS, high), 0)
    order = lax.broadcasted_iota(jnp.int32, (COLS, wide), 0)
    fine_cols = col * COLS + (order & (SEGS - 1)) * SEG + (order >> 3)
    row_mat[...] = interp_block(fine_rows, start, total_rows, (ROWS, high)).astype(bf16)
    col_mat[...] = interp_block(fine_cols, begin, total_cols, (COLS, wide)).astype(bf16)


def upsampled_tile(cb, row_mat, col_mat, total_rows, total_cols):
    high, wide = cb.shape[1:]
    start, _ = coarse_window(total_cols, wide)
    disp, conf = cb[0], cb[1]
    place = lax.broadcasted_iota(jnp.int32, (high, wide), 0) + start
    lane = lax.broadcasted_iota(jnp.int32, (high, wide), 1)
    good = (place >= 0) & (place < total_rows)
    local = lax.broadcasted_iota(jnp.int32, (high, wide), 0)
    pull = conf * disp
    current = disp
    for _ in range(CITER):
        up = jnp.where(local == 0, 0.0, pltpu.roll(current, 1, 0))
        down = jnp.where(local == high - 1, 0.0, pltpu.roll(current, high - 1, 0))
        left = jnp.where(lane == 0, 0.0, pltpu.roll(current, 1, 1))
        right = jnp.where(lane == wide - 1, 0.0, pltpu.roll(current, wide - 1, 1))
        current = jnp.where(good, (pull + (up + down + left + right)) / (conf + 4.0), 0.0)
    tall = jnp.zeros((ROWS, wide), f32)
    for piece in parts(current, 3):
        tall += jnp.dot(row_mat[...], piece, preferred_element_type=f32)
    out = jnp.zeros((COLS, ROWS), f32)
    for piece in parts(tall, 3):
        out += lax.dot_general(col_mat[...], piece, (((1,), (1,)), ((), ())), preferred_element_type=f32)
    return out


MESH = pl.DeviceIdType.MESH


def stereo_kernel(coarse_shape, ids, ref_in, src_in, hyp_in, disp_in, conf_in, out,
                  img, hyp, coarse, xm, hal, cb, ht, htc, sel, up, red, border, tmp, near,
                  xs, hs, rt, rx3, rmom, xmom, lmom, cmom, av, bv, lhs, lx, yy, vol, zt, row_mat, col_mat,
                  load, local, send, recv, csend, crecv):
    row, col = lax.axis_index("row"), lax.axis_index("col")
    nr, nc = lax.axis_size("row"), lax.axis_size("col")
    wide = cb.shape[2]
    last = (coarse_shape[1] - wide) // 128

    loads = [
        pltpu.make_async_copy(ref_in, img.at[0], load.at[0]),
        pltpu.make_async_copy(src_in, img.at[pl.ds(1, SRC)], load.at[1]),
        pltpu.make_async_copy(disp_in, coarse.at[0], load.at[2]),
        pltpu.make_async_copy(conf_in, coarse.at[1], load.at[3]),
        pltpu.make_async_copy(hyp_in, hyp, load.at[4]),
    ]
    for copy in loads:
        copy.start()

    def inside(dr, dc):
        good = row >= 0
        if dr:
            good = good & ((row > 0) if dr < 0 else (row < nr - 1))
        if dc:
            good = good & ((col > 0) if dc < 0 else (col < nc - 1))
        return good

    def away(dr, dc):
        return {"row": lax.rem(row + dr + nr, nr), "col": lax.rem(col + dc + nc, nc)}

    around = [(dr, dc) for dr in (-1, 0, 1) for dc in (-1, 0, 1) if dr or dc]
    odd = lax.rem(row, 2)
    main_col = row // 2
    side_col = main_col - 1 + 2 * odd
    side_there = (side_col >= 0) & (side_col < nc)
    is_main = col == main_col
    is_side = col == side_col

    barrier = pltpu.get_barrier_semaphore()
    expected = jnp.int32(0)
    for dr, dc in around:
        expected += inside(dr, dc).astype(jnp.int32)

        @pl.when(inside(dr, dc))
        def _(dr=dr, dc=dc):
            pl.semaphore_signal(barrier, inc=1, device_id=away(dr, dc), device_id_type=MESH)

    @pl.when(jnp.logical_not(is_main))
    def _():
        pl.semaphore_signal(barrier, inc=1, device_id={"row": row, "col": main_col}, device_id_type=MESH)

    @pl.when(side_there & jnp.logical_not(is_side))
    def _():
        pl.semaphore_signal(barrier, inc=1, device_id={"row": row, "col": jnp.clip(side_col, 0, nc - 1)}, device_id_type=MESH)

    expected += (nc - 1) * (is_main.astype(jnp.int32) + is_side.astype(jnp.int32))
    copies = []

    def push(dr, dc, source, target):
        n = len(copies)
        copy = pltpu.make_async_remote_copy(source, target, send.at[n], recv.at[n], device_id=away(dr, dc), device_id_type=MESH)
        copies.append((dr, dc, copy, target))

        @pl.when(inside(dr, dc))
        def _():
            copy.start()

    def arrive(entries):
        for dr, dc, copy, target in entries:
            @pl.when(inside(-dr, -dc))
            def _(copy=copy):
                copy.wait_recv()

            @pl.when(jnp.logical_not(inside(-dr, -dc)))
            def _(target=target):
                target[...] = jnp.zeros(target.shape, f32)

    def leave(entries):
        for dr, dc, copy, target in entries:
            @pl.when(inside(dr, dc))
            def _(copy=copy):
                copy.wait_send()

    loads[0].wait()
    loads[1].wait()
    for v in range(SRC + 1):
        xm[v, PADL:PADL + COLS, :] = img[v].T
    pl.semaphore_wait(barrier, expected)
    for dc in (1, -1, 0):
        lanes = {0: (0, COLS), 1: (COLS - 128, 128), -1: (0, 128)}[dc]
        to = {0: 128, 1: 0, -1: 384}[dc]
        for dr in (1, -1):
            here = pl.ds(ROWS - 8, 8) if dr == 1 else pl.ds(0, 8)
            side = 0 if dr == 1 else 1
            push(dr, dc, img.at[:, here, pl.ds(*lanes)], hal.at[side, :, :, pl.ds(to, lanes[1])])

    push(0, 1, xm.at[pl.ds(1, SRC), pl.ds(COLS, PADL), :], xm.at[pl.ds(1, SRC), pl.ds(0, PADL), :])
    push(0, -1, xm.at[:, pl.ds(PADL, 8), :], xm.at[:, pl.ds(PADL + COLS, 8), :])
    push(0, 1, xm.at[pl.ds(0, 1), pl.ds(PADL + COLS - 8, 8), :], xm.at[pl.ds(0, 1), pl.ds(PADL - 8, 8), :])
    halos = list(copies)

    loads[2].wait()
    loads[3].wait()
    main_src = pl.ds(pl.multiple_of(8 * odd, 8), 24)
    main_dst = cb.at[:, pl.ds(pl.multiple_of(8 - 8 * odd, 8), 24), :]
    side_src = pl.ds(pl.multiple_of(24 - 24 * odd, 8), 8)
    side_dst = cb.at[:, pl.ds(pl.multiple_of(24 * odd, 8), 8), :]

    def coarse_copy(j, rows, target, kind):
        lanes = pl.ds(pl.multiple_of(128 * jnp.clip((32 * j + 123) // 128 - 1, 0, last), 128), wide)
        source = coarse.at[:, rows, lanes]
        return pltpu.make_async_remote_copy(source, target, csend.at[j], crecv.at[kind], device_id={"row": row, "col": j}, device_id_type=MESH)

    def coarse_own(rows, target):
        lanes = pl.ds(pl.multiple_of(128 * jnp.clip((32 * col + 123) // 128 - 1, 0, last), 128), wide)
        return pltpu.make_async_copy(coarse.at[:, rows, lanes], target, local.at[0])

    loads[4].wait()
    interp_mats(row_mat, col_mat, *coarse_shape)
    packed = hyp[0]
    for k in range(1, HYP):
        packed = packed | (hyp[k] << (4 * k))
    htc[...] = packed.T
    for i in range(SEG):
        ht[8 * i:8 * i + 8, :] = htc[pl.ds(i, SEGS, stride=SEG), :]

    zero = jnp.zeros((128, 128), bf16)
    b = band_main()
    halo = [band_halo(v) for v in range(SRC)]
    rt[0:128, 0:128] = b
    rt[0:128, 128:256] = zero
    rt[128:256, 0:128] = zero
    rt[128:256, 128:256] = b
    for v in range(SRC):
        rmom[v, 0:128, 0:128] = halo[v]
        rmom[v, 0:128, 128:256] = zero
        rmom[v, 128:256, 0:128] = zero
        rmom[v, 128:256, 128:256] = halo[v]
        p, q = v // 2, v % 2
        rx3[p, 0:128, 128 * q:128 * q + 128] = halo[v]
        rx3[p, 128:256, 128 * q:128 * q + 128] = halo[v]


    for j in range(NJ):
        for v in range(SRC + 1):
            if v or j >= SHIFT:
                lo = 2 if j < LEFT - SEG else 1 if j < LEFT else 0
                hi = SEGS - 1 if j >= NJ - R else SEGS
                at = lo * SEG + j + PADL - LEFT
                xs[v, j, lo:hi, :] = xm[v, pl.ds(at, hi - lo, stride=SEG), :]

    arrive(halos)
    kinds = ((is_main, main_src, main_dst, 0), (is_side, side_src, side_dst, 1))
    for role, rows, target, kind in kinds:
        @pl.when(role)
        def _(rows=rows, target=target, kind=kind):
            def one(j, carry):
                @pl.when(j != col)
                def _():
                    coarse_copy(j, rows, target, kind).start()

                return carry

            lax.fori_loop(0, nc, one, 0)
            coarse_own(rows, target).start()

    gap = jnp.zeros((64 - SRC * HL, 512), f32)
    stack = []
    for v in range(SRC):
        stack += [hal[0, v + 1, 8 - R:8, :], hal[1, v + 1, 0:R, :]]
    stack.append(gap)
    for v in range(SRC):
        stack += [hal[0, 0, 8 - R:8, :], hal[1, 0, 0:R, :]]
    stack.append(gap)
    zt[...] = jnp.concatenate(stack, axis=0).T
    for j in range(NJ):
        if j < LEFT:
            for v in range(SRC):
                xs[v + 1, j, 0:1, :] = xm[v + 1, j + PADL - LEFT:j + PADL - LEFT + 1, :]
                if j < LEFT - SEG:
                    at = SEG + j + PADL - LEFT
                    xs[v + 1, j, 1:2, :] = xm[v + 1, at:at + 1, :]
        if SHIFT <= j < LEFT:
            xs[0, j, 0:1, :] = xm[0, j + PADL - LEFT:j + PADL - LEFT + 1, :]
        if j >= NJ - R:
            at = (SEGS - 1) * SEG + j + PADL - LEFT
            for v in range(SRC + 1):
                xs[v, j, SEGS - 1:SEGS, :] = xm[v, at:at + 1, :]
        edge = zt[pl.ds(j + 128 - LEFT, SEGS, stride=SEG), :]
        hs[1, j] = edge
        if j >= SHIFT:
            hs[0, j] = pltpu.roll(edge, 64, 1)

    def moments(load, first, count, ref):
        vals = [load(first + j) for j in range(count)]
        put_parts(ref, window11(vals), (0, 256, 512))
        vals = [load(first + j) for j in range(count)]
        put_parts(ref, window11([x * x for x in vals]), (128, 384, 640))

    def finish(rows, view):
        total = jnp.dot(lmom[0:rows, 0:256], rt[...], preferred_element_type=f32)
        for t in (256, 512):
            total += jnp.dot(lmom[0:rows, t:t + 256], rt[...], preferred_element_type=f32)
        for t in (0, 256, 512):
            total += jnp.dot(xmom[0:rows, t:t + 256], rmom[view], preferred_element_type=f32)
        cmom[0:rows, :] = total

    moments(lambda j: hs[0, j], SHIFT, NK, xmom)
    moments(lambda j: xs[0, j], SHIFT, NK, lmom)
    finish(SEG * 8, 0)
    for i in range(SEG):
        m = cmom[8 * i:8 * i + 8, 0:128] / AREA
        var = cmom[8 * i:8 * i + 8, 128:256] / AREA - m * m + FLOOR
        av[0, i] = lax.rsqrt(var)
        bv[0, i] = m

    moments(lambda j: hs[1, j], 0, NJ, xmom)

    def view_moments(v, carry):
        moments(lambda j: xs[v + 1, j], 0, NJ, lmom)
        finish(NM * 8, v)

        for i in range(NM):
            rows = slice(8 * i, 8 * i + 8)
            m = cmom[rows, 0:128] / AREA
            var = cmom[rows, 128:256] / AREA - m * m + FLOOR
            inv = lax.rsqrt(var) / SRC
            av[v + 1, i] = inv / AREA
            bv[v + 1, i] = m * inv
        return carry

    lax.fori_loop(0, SRC, view_moments, 0)

    lane = lax.broadcasted_iota(jnp.int32, (8, 128), 1)
    masks = [lane < HL * (v + 1) for v in range(SRC - 1)]

    def level(step, carry):
        starts = []
        for u in range(LB):
            l = LB * step + u
            begins = [SHIFT - ids[v] * l for v in range(SRC)]
            starts.append((l, begins))
            pieces = [hs[1, pl.ds(begins[v], NK)] for v in range(SRC)]
            prods = []
            for k in range(NK):
                piece = pieces[3][k]
                for v in (2, 1, 0):
                    piece = jnp.where(masks[v], pieces[v][k], piece)
                prods.append(hs[0, SHIFT + k] * piece)
            part = pl.ds(256 * u, 256)
            put_parts(lx.at[part], window11(prods), (0, 128))
            for v in range(SRC):
                moved = xs[v + 1, pl.ds(begins[v], NK)]
                prods = [xs[0, SHIFT + k] * moved[k] for k in range(NK)]
                put_parts(lhs.at[v // 2, part], window11(prods), (128 * (v % 2), 256 + 128 * (v % 2)))
        for p in range(SRC // 2):
            total = jnp.dot(lhs[p, :, 0:256], rt[...], preferred_element_type=f32)
            total += jnp.dot(lhs[p, :, 256:512], rt[...], preferred_element_type=f32)
            total += jnp.dot(lx[...], rx3[p], preferred_element_type=f32)
            yy[p] = total
        for u in range(LB):
            l, begins = starts[u]
            scale = [av[v + 1, pl.ds(begins[v], SEG)] for v in range(SRC)]
            shift = [bv[v + 1, pl.ds(begins[v], SEG)] for v in range(SRC)]
            for i in range(SEG):
                rows = slice(256 * u + 8 * i, 256 * u + 8 * i + 8)
                acc = None
                sub = None
                for v in range(SRC):
                    y = yy[v // 2, rows, 128 * (v % 2):128 * (v % 2) + 128]
                    a = y * scale[v][i]
                    s = shift[v][i]
                    acc = a if acc is None else acc + a
                    sub = s if sub is None else sub + s
                vol[l, i] = av[0, i] * (acc - bv[0, i] * sub)
        return carry

    lax.fori_loop(0, LEVELS // LB, level, 0)

    for role, rows, target, kind in kinds:
        there = side_there if kind else col >= 0

        @pl.when(role)
        def _(rows=rows, target=target, kind=kind):
            coarse_own(rows, target).wait()

        @pl.when(jnp.logical_not(role) & there)
        def _(rows=rows, target=target, kind=kind):
            coarse_copy(col, rows, target, kind).wait_recv()

    @pl.when(jnp.logical_not(side_there))
    def _():
        side_dst[...] = jnp.zeros(side_dst.shape, f32)

    up[...] = upsampled_tile(cb, row_mat, col_mat, *coarse_shape)

    def pick(i, carry):
        rows = pl.ds(pl.multiple_of(8 * i, 8), 8)
        codes = ht[rows, :]
        centre = up[rows, :]
        num = jnp.zeros((8, 128), f32)
        den = jnp.zeros((8, 128), f32)
        for k in range(HYP):
            table = [vol[l, i] for l in range(LEVELS)]
            for bit in range(4):
                odd = (codes & jnp.int32((1 << (4 * k + bit)) - (1 << 32 if 4 * k + bit == 31 else 0))) != 0
                table = [jnp.where(odd, table[t + 1], table[t]) for t in range(0, len(table), 2)]
            gain = 10.0 * table[0] - 10.0
            sel[k, rows, :] = gain
            cand = (lax.shift_right_logical(codes, 4 * k) & 15).astype(f32)
            d = cand - centre
            w = jnp.exp(gain - 0.1 * (d * d))
            num += w * cand
            den += w
        red[rows, :] = num / den
        return carry

    lax.fori_loop(0, SEG, pick, 0)


    lane = lax.broadcasted_iota(jnp.int32, (8, 128), 1)
    edge = jnp.zeros((8, 128), f32)
    for i in range(SEG):
        v = red[8 * i:8 * i + 8, :]
        edge = jnp.where(lane == i, jnp.broadcast_to(v[:, 0:1], (8, 128)), edge)
        edge = jnp.where(lane == SEG + i, jnp.broadcast_to(v[:, 127:128], (8, 128)), edge)
    border[...] = edge


    copies.clear()
    copies.extend(halos)
    push(0, 1, red.at[pl.ds(8 * SEG - 8, 8), :], near.at[2])
    push(0, -1, red.at[pl.ds(0, 8), :], near.at[3])
    push(1, 0, border, near.at[0])
    push(-1, 0, border, near.at[1])
    final = copies[len(halos):]

    leave(halos)
    for role, rows, target, kind in kinds:
        @pl.when(role)
        def _(rows=rows, target=target, kind=kind):
            def one(j, carry):
                @pl.when(j != col)
                def _():
                    coarse_copy(j, rows, target, kind).wait_send()

                return carry

            lax.fori_loop(0, nc, one, 0)

    arrive(final)
    lane = lax.broadcasted_iota(jnp.int32, (8, 128), 1)
    seg = lax.broadcasted_iota(jnp.int32, (8, 128), 0)
    row_edge = jnp.where((lane == 0) & (row == 0), 1.0, 0.0) + jnp.where(
        (lane == ROWS - 1) & (row == nr - 1), 1.0, 0.0)
    above_v = near[0]
    below_v = near[1]
    left, right = near.at[2], near.at[3]
    for i in range(SEG):
        rows = slice(8 * i, 8 * i + 8)
        r = red[rows, :]
        u = up[rows, :]
        h = ht[rows, :]
        north = jnp.where(lane == 0, jnp.broadcast_to(above_v[:, SEG + i:SEG + i + 1], (8, 128)), pltpu.roll(r, 1, 1))
        south = jnp.where(lane == ROWS - 1, jnp.broadcast_to(below_v[:, i:i + 1], (8, 128)), pltpu.roll(r, ROWS - 1, 1))
        if i == 0:
            west = jnp.concatenate([left[7:8, :], red[8 * SEG - 8:8 * SEG - 1, :]], axis=0)
        else:
            west = red[8 * i - 8:8 * i, :]
        if i == SEG - 1:
            east = jnp.concatenate([red[1:8, :], right[0:1, :]], axis=0)
        else:
            east = red[8 * i + 8:8 * i + 16, :]
        count = 4.0 - row_edge
        if i == 0:
            count = count - jnp.where((seg == 0) & (col == 0), 1.0, 0.0)
        if i == SEG - 1:
            count = count - jnp.where((seg == 7) & (col == nc - 1), 1.0, 0.0)
        centre = 0.5 * u + 0.5 * (north + south + west + east) / count
        num = jnp.zeros((8, 128), f32)
        den = jnp.zeros((8, 128), f32)
        for k in range(HYP):
            cand = (lax.shift_right_logical(h, 4 * k) & 15).astype(f32)
            d = cand - centre
            w = jnp.exp(sel[k, rows, :] - 0.1 * (d * d))
            num += w * cand
            den += w
        even = ((lane + i) & 1) == 0
        tmp[pl.ds(i, SEGS, stride=SEG), :] = jnp.where(even, r, num / den)
    out[...] = tmp[...].T
    leave(final)


def on_device(reference_image, source_images, hypotheses, source_ids, coarse_disp, coarse_conf):
    shape = (coarse_disp.shape[0] * lax.axis_size("col"), coarse_disp.shape[1])
    anywhere = pl.BlockSpec(memory_space=pltpu.HBM)
    n = SEG * 8
    return pl.pallas_call(
        functools.partial(stereo_kernel, shape),
        out_shape=jax.ShapeDtypeStruct((ROWS, COLS), f32),
        in_specs=[pl.BlockSpec(memory_space=pltpu.SMEM)] + [anywhere] * 5,
        out_specs=pl.BlockSpec(memory_space=pltpu.VMEM),
        scratch_shapes=[
            pltpu.VMEM((SRC + 1, ROWS, COLS), f32),
            pltpu.VMEM((HYP, ROWS, COLS), jnp.int32),
            pltpu.VMEM((2,) + coarse_disp.shape, f32),
            pltpu.VMEM((SRC + 1, CI, 128), f32),
            pltpu.VMEM((2, SRC + 1, 8, 512), f32),
            pltpu.VMEM((2, 32, min(256, coarse_disp.shape[1])), f32),
            pltpu.VMEM((n, 128), jnp.int32),
            pltpu.VMEM((COLS, ROWS), jnp.int32),
            pltpu.VMEM((HYP, n, 128), f32),
            pltpu.VMEM((n, 128), f32),
            pltpu.VMEM((n, 128), f32),
            pltpu.VMEM((8, 128), f32),
            pltpu.VMEM((COLS, ROWS), f32),
            pltpu.VMEM((4, 8, 128), f32),
            pltpu.VMEM((SRC + 1, NJ, 8, 128), f32),
            pltpu.VMEM((2, NJ, 8, 128), f32),
            pltpu.VMEM((256, 256), bf16),
            pltpu.VMEM((2, 256, 256), bf16),
            pltpu.VMEM((SRC, 256, 256), bf16),
            pltpu.VMEM((NM * 8 + 8, 768), bf16),
            pltpu.VMEM((NM * 8 + 8, 768), bf16),
            pltpu.VMEM((NM * 8, 256), f32),
            pltpu.VMEM((SRC + 1, NM, 8, 128), f32),
            pltpu.VMEM((SRC + 1, NM, 8, 128), f32),
            pltpu.VMEM((2, LB * n, 512), bf16),
            pltpu.VMEM((LB * n, 256), bf16),
            pltpu.VMEM((2, LB * n, 256), f32),
            pltpu.VMEM((LEVELS, SEG, 8, 128), f32),
            pltpu.VMEM((512, 128), f32),
            pltpu.VMEM((ROWS, 32), bf16),
            pltpu.VMEM((COLS, min(256, coarse_disp.shape[1])), bf16),
            pltpu.SemaphoreType.DMA((5,)),
            pltpu.SemaphoreType.DMA((1,)),
            pltpu.SemaphoreType.DMA((13,)),
            pltpu.SemaphoreType.DMA((13,)),
            pltpu.SemaphoreType.DMA((16,)),
            pltpu.SemaphoreType.DMA((2,)),
        ],
        compiler_params=pltpu.CompilerParams(
            collective_id=0, has_side_effects=True, vmem_limit_bytes=VMEM_LIMIT),
    )(source_ids, reference_image, source_images, hypotheses, coarse_disp, coarse_conf)


def solution(mesh):
    in_specs = (
        P("row", "col"),
        P(None, "row", "col"),
        P(None, "row", "col"),
        P(),
        P("col", None),
        P("col", None),
    )
    return jax.shard_map(
        on_device, mesh=mesh, in_specs=in_specs, out_specs=P("row", "col"), check_vma=False
    )
```

```python
import functools

import jax
import jax.numpy as jnp
from jax import lax
from jax.experimental import pallas as pl
from jax.experimental.pallas import tpu as pltpu
from jax.sharding import PartitionSpec as P

LEVELS = 16
HYP = 8
SRC = 4
MAXID = 3
WIN = 11
UPS = 8
CITER = 4
R = WIN // 2
AREA = float(WIN * WIN)
FLOOR = 1e-05

ROWS, COLS = 128, 256
SEGS = 8
SEG = COLS // SEGS
SHIFT = MAXID * (LEVELS - 1)
LEFT = SHIFT + R
PADL = 56
CI = 320
NJ = SEG + 2 * R + SHIFT
NK = SEG + 2 * R
NM = SEG + SHIFT
HL = 2 * R
LB = 4
VMEM_LIMIT = 60 * 1024 * 1024
bf16 = jnp.bfloat16
f32 = jnp.float32


def window11(vals):
    n = len(vals)
    count = n - WIN + 1
    suf, pre = {}, {}
    for start in range(0, n, WIN):
        stop = min(start + WIN, n)
        if stop - start == WIN and start < count:
            acc = vals[stop - 1]
            suf[stop - 1] = acc
            for i in range(stop - 2, start - 1, -1):
                acc = vals[i] + acc
                suf[i] = acc
        if start:
            acc = vals[start]
            pre[start] = acc
            for i in range(start + 1, min(stop, start + WIN - 1)):
                acc = acc + vals[i]
                pre[i] = acc
    return [suf[i] if i % WIN == 0 else suf[i] + pre[i + WIN - 1] for i in range(count)]


def parts(value, count):
    out = []
    for _ in range(count - 1):
        piece = value.astype(bf16)
        out.append(piece)
        value = value - piece.astype(f32)
    out.append(value.astype(bf16))
    return out


def put_parts(ref, sums, columns):
    n = len(sums)
    for q in range(0, n, 2):
        both = jnp.concatenate(sums[q:q + 2], axis=0) if q + 1 < n else sums[q]
        for piece, col in zip(parts(both, len(columns)), columns):
            ref[8 * q:8 * q + both.shape[0], col:col + 128] = piece


def band_main():
    a = lax.broadcasted_iota(jnp.int32, (ROWS, ROWS), 0)
    b = lax.broadcasted_iota(jnp.int32, (ROWS, ROWS), 1)
    return jnp.where(jnp.abs(a - b) <= R, 1.0, 0.0).astype(bf16)


def band_halo(view):
    a = lax.broadcasted_iota(jnp.int32, (128, ROWS), 0) - view * HL
    b = lax.broadcasted_iota(jnp.int32, (128, ROWS), 1)
    row = jnp.where(a < R, a - R, a - R + ROWS)
    good = (a >= 0) & (a < HL) & (jnp.abs(row - b) <= R)
    return jnp.where(good, 1.0, 0.0).astype(bf16)


def interp_block(fine, coarse_start, total, shape):
    numerator = 2 * fine + 1 - UPS
    lower = numerator >> 4
    fraction = (numerator - lower * 2 * UPS).astype(f32) / (2.0 * UPS)
    where = lax.broadcasted_iota(jnp.int32, shape, 1) + coarse_start
    low = jnp.where(where == jnp.clip(lower, 0, total - 1), 1.0 - fraction, 0.0)
    high = jnp.where(where == jnp.clip(lower + 1, 0, total - 1), fraction, 0.0)
    return low + high


def coarse_window(total_cols, wide):
    row, col = lax.axis_index("row"), lax.axis_index("col")
    return 16 * row - 8, 128 * jnp.clip((32 * col + 123) // 128 - 1, 0, (total_cols - wide) // 128)


def interp_mats(row_mat, col_mat, total_rows, total_cols):
    row, col = lax.axis_index("row"), lax.axis_index("col")
    high, wide = row_mat.shape[1], col_mat.shape[1]
    start, begin = coarse_window(total_cols, wide)
    fine_rows = row * ROWS + lax.broadcasted_iota(jnp.int32, (ROWS, high), 0)
    order = lax.broadcasted_iota(jnp.int32, (COLS, wide), 0)
    fine_cols = col * COLS + (order & (SEGS - 1)) * SEG + (order >> 3)
    row_mat[...] = interp_block(fine_rows, start, total_rows, (ROWS, high)).astype(bf16)
    col_mat[...] = interp_block(fine_cols, begin, total_cols, (COLS, wide)).astype(bf16)


def upsampled_tile(cb, row_mat, col_mat, total_rows, total_cols):
    high, wide = cb.shape[1:]
    start, _ = coarse_window(total_cols, wide)
    disp, conf = cb[0], cb[1]
    place = lax.broadcasted_iota(jnp.int32, (high, wide), 0) + start
    lane = lax.broadcasted_iota(jnp.int32, (high, wide), 1)
    good = (place >= 0) & (place < total_rows)
    local = lax.broadcasted_iota(jnp.int32, (high, wide), 0)
    pull = conf * disp
    current = disp
    for _ in range(CITER):
        up = jnp.where(local == 0, 0.0, pltpu.roll(current, 1, 0))
        down = jnp.where(local == high - 1, 0.0, pltpu.roll(current, high - 1, 0))
        left = jnp.where(lane == 0, 0.0, pltpu.roll(current, 1, 1))
        right = jnp.where(lane == wide - 1, 0.0, pltpu.roll(current, wide - 1, 1))
        current = jnp.where(good, (pull + (up + down + left + right)) / (conf + 4.0), 0.0)
    tall = jnp.zeros((ROWS, wide), f32)
    for piece in parts(current, 3):
        tall += jnp.dot(row_mat[...], piece, preferred_element_type=f32)
    out = jnp.zeros((COLS, ROWS), f32)
    for piece in parts(tall, 3):
        out += lax.dot_general(col_mat[...], piece, (((1,), (1,)), ((), ())), preferred_element_type=f32)
    return out


MESH = pl.DeviceIdType.MESH


def stereo_kernel(coarse_shape, ids, ref_in, src_in, hyp_in, disp_in, conf_in, out,
                  img, hyp, coarse, xm, hal, cb, ht, htc, sel, up, red, border, tmp, near,
                  xs, hs, rt, rx3, rmom, xmom, lmom, cmom, av, bv, lhs, lx, yy, vol, zt, row_mat, col_mat,
                  load, local, send, recv, csend, crecv):
    row, col = lax.axis_index("row"), lax.axis_index("col")
    nr, nc = lax.axis_size("row"), lax.axis_size("col")
    wide = cb.shape[2]
    last = (coarse_shape[1] - wide) // 128

    loads = [
        pltpu.make_async_copy(ref_in, img.at[0], load.at[0]),
        pltpu.make_async_copy(src_in, img.at[pl.ds(1, SRC)], load.at[1]),
        pltpu.make_async_copy(disp_in, coarse.at[0], load.at[2]),
        pltpu.make_async_copy(conf_in, coarse.at[1], load.at[3]),
        pltpu.make_async_copy(hyp_in, hyp, load.at[4]),
    ]
    for copy in loads:
        copy.start()

    def inside(dr, dc):
        good = row >= 0
        if dr:
            good = good & ((row > 0) if dr < 0 else (row < nr - 1))
        if dc:
            good = good & ((col > 0) if dc < 0 else (col < nc - 1))
        return good

    def away(dr, dc):
        return {"row": lax.rem(row + dr + nr, nr), "col": lax.rem(col + dc + nc, nc)}

    around = [(dr, dc) for dr in (-1, 0, 1) for dc in (-1, 0, 1) if dr or dc]
    odd = lax.rem(row, 2)
    main_col = row // 2
    side_col = main_col - 1 + 2 * odd
    side_there = (side_col >= 0) & (side_col < nc)
    is_main = col == main_col
    is_side = col == side_col

    barrier = pltpu.get_barrier_semaphore()
    expected = jnp.int32(0)
    for dr, dc in around:
        expected += inside(dr, dc).astype(jnp.int32)

        @pl.when(inside(dr, dc))
        def _(dr=dr, dc=dc):
            pl.semaphore_signal(barrier, inc=1, device_id=away(dr, dc), device_id_type=MESH)

    @pl.when(jnp.logical_not(is_main))
    def _():
        pl.semaphore_signal(barrier, inc=1, device_id={"row": row, "col": main_col}, device_id_type=MESH)

    @pl.when(side_there & jnp.logical_not(is_side))
    def _():
        pl.semaphore_signal(barrier, inc=1, device_id={"row": row, "col": jnp.clip(side_col, 0, nc - 1)}, device_id_type=MESH)

    expected += (nc - 1) * (is_main.astype(jnp.int32) + is_side.astype(jnp.int32))
    copies = []

    def push(dr, dc, source, target):
        n = len(copies)
        copy = pltpu.make_async_remote_copy(source, target, send.at[n], recv.at[n], device_id=away(dr, dc), device_id_type=MESH)
        copies.append((dr, dc, copy, target))

        @pl.when(inside(dr, dc))
        def _():
            copy.start()

    def arrive(entries):
        for dr, dc, copy, target in entries:
            @pl.when(inside(-dr, -dc))
            def _(copy=copy):
                copy.wait_recv()

            @pl.when(jnp.logical_not(inside(-dr, -dc)))
            def _(target=target):
                target[...] = jnp.zeros(target.shape, f32)

    def leave(entries):
        for dr, dc, copy, target in entries:
            @pl.when(inside(dr, dc))
            def _(copy=copy):
                copy.wait_send()

    loads[0].wait()
    loads[1].wait()
    for v in range(SRC + 1):
        xm[v, PADL:PADL + COLS, :] = img[v].T
    pl.semaphore_wait(barrier, expected)
    for dc in (1, -1, 0):
        lanes = {0: (0, COLS), 1: (COLS - 128, 128), -1: (0, 128)}[dc]
        to = {0: 128, 1: 0, -1: 384}[dc]
        for dr in (1, -1):
            here = pl.ds(ROWS - 8, 8) if dr == 1 else pl.ds(0, 8)
            side = 0 if dr == 1 else 1
            push(dr, dc, img.at[:, here, pl.ds(*lanes)], hal.at[side, :, :, pl.ds(to, lanes[1])])

    push(0, 1, xm.at[pl.ds(1, SRC), pl.ds(COLS, PADL), :], xm.at[pl.ds(1, SRC), pl.ds(0, PADL), :])
    push(0, -1, xm.at[:, pl.ds(PADL, 8), :], xm.at[:, pl.ds(PADL + COLS, 8), :])
    push(0, 1, xm.at[pl.ds(0, 1), pl.ds(PADL + COLS - 8, 8), :], xm.at[pl.ds(0, 1), pl.ds(PADL - 8, 8), :])
    halos = list(copies)

    loads[2].wait()
    loads[3].wait()
    main_src = pl.ds(pl.multiple_of(8 * odd, 8), 24)
    main_dst = cb.at[:, pl.ds(pl.multiple_of(8 - 8 * odd, 8), 24), :]
    side_src = pl.ds(pl.multiple_of(24 - 24 * odd, 8), 8)
    side_dst = cb.at[:, pl.ds(pl.multiple_of(24 * odd, 8), 8), :]

    def coarse_copy(j, rows, target, kind):
        lanes = pl.ds(pl.multiple_of(128 * jnp.clip((32 * j + 123) // 128 - 1, 0, last), 128), wide)
        source = coarse.at[:, rows, lanes]
        return pltpu.make_async_remote_copy(source, target, csend.at[j], crecv.at[kind], device_id={"row": row, "col": j}, device_id_type=MESH)

    def coarse_own(rows, target):
        lanes = pl.ds(pl.multiple_of(128 * jnp.clip((32 * col + 123) // 128 - 1, 0, last), 128), wide)
        return pltpu.make_async_copy(coarse.at[:, rows, lanes], target, local.at[0])

    loads[4].wait()
    interp_mats(row_mat, col_mat, *coarse_shape)
    packed = hyp[0]
    for k in range(1, HYP):
        packed = packed | (hyp[k] << (4 * k))
    htc[...] = packed.T
    for i in range(SEG):
        ht[8 * i:8 * i + 8, :] = htc[pl.ds(i, SEGS, stride=SEG), :]

    zero = jnp.zeros((128, 128), bf16)
    b = band_main()
    halo = [band_halo(v) for v in range(SRC)]
    rt[0:128, 0:128] = b
    rt[0:128, 128:256] = zero
    rt[128:256, 0:128] = zero
    rt[128:256, 128:256] = b
    for v in range(SRC):
        rmom[v, 0:128, 0:128] = halo[v]
        rmom[v, 0:128, 128:256] = zero
        rmom[v, 128:256, 0:128] = zero
        rmom[v, 128:256, 128:256] = halo[v]
        p, q = v // 2, v % 2
        rx3[p, 0:128, 128 * q:128 * q + 128] = halo[v]
        rx3[p, 128:256, 128 * q:128 * q + 128] = halo[v]


    for j in range(NJ):
        for v in range(SRC + 1):
            if v or j >= SHIFT:
                lo = 2 if j < LEFT - SEG else 1 if j < LEFT else 0
                hi = SEGS - 1 if j >= NJ - R else SEGS
                at = lo * SEG + j + PADL - LEFT
                xs[v, j, lo:hi, :] = xm[v, pl.ds(at, hi - lo, stride=SEG), :]

    arrive(halos)
    kinds = ((is_main, main_src, main_dst, 0), (is_side, side_src, side_dst, 1))
    for role, rows, target, kind in kinds:
        @pl.when(role)
        def _(rows=rows, target=target, kind=kind):
            def one(j, carry):
                @pl.when(j != col)
                def _():
                    coarse_copy(j, rows, target, kind).start()

                return carry

            lax.fori_loop(0, nc, one, 0)
            coarse_own(rows, target).start()

    gap = jnp.zeros((64 - SRC * HL, 512), f32)
    stack = []
    for v in range(SRC):
        stack += [hal[0, v + 1, 8 - R:8, :], hal[1, v + 1, 0:R, :]]
    stack.append(gap)
    for v in range(SRC):
        stack += [hal[0, 0, 8 - R:8, :], hal[1, 0, 0:R, :]]
    stack.append(gap)
    zt[...] = jnp.concatenate(stack, axis=0).T
    for j in range(NJ):
        if j < LEFT:
            for v in range(SRC):
                xs[v + 1, j, 0:1, :] = xm[v + 1, j + PADL - LEFT:j + PADL - LEFT + 1, :]
                if j < LEFT - SEG:
                    at = SEG + j + PADL - LEFT
                    xs[v + 1, j, 1:2, :] = xm[v + 1, at:at + 1, :]
        if SHIFT <= j < LEFT:
            xs[0, j, 0:1, :] = xm[0, j + PADL - LEFT:j + PADL - LEFT + 1, :]
        if j >= NJ - R:
            at = (SEGS - 1) * SEG + j + PADL - LEFT
            for v in range(SRC + 1):
                xs[v, j, SEGS - 1:SEGS, :] = xm[v, at:at + 1, :]
        edge = zt[pl.ds(j + 128 - LEFT, SEGS, stride=SEG), :]
        hs[1, j] = edge
        if j >= SHIFT:
            hs[0, j] = pltpu.roll(edge, 64, 1)

    def moments(load, first, count, ref):
        vals = [load(first + j) for j in range(count)]
        put_parts(ref, window11(vals), (0, 256, 512))
        vals = [load(first + j) for j in range(count)]
        put_parts(ref, window11([x * x for x in vals]), (128, 384, 640))

    def finish(rows, view):
        total = jnp.dot(lmom[0:rows, 0:256], rt[...], preferred_element_type=f32)
        for t in (256, 512):
            total += jnp.dot(lmom[0:rows, t:t + 256], rt[...], preferred_element_type=f32)
        for t in (0, 256, 512):
            total += jnp.dot(xmom[0:rows, t:t + 256], rmom[view], preferred_element_type=f32)
        cmom[0:rows, :] = total

    moments(lambda j: hs[0, j], SHIFT, NK, xmom)
    moments(lambda j: xs[0, j], SHIFT, NK, lmom)
    finish(SEG * 8, 0)
    for i in range(SEG):
        m = cmom[8 * i:8 * i + 8, 0:128] / AREA
        var = cmom[8 * i:8 * i + 8, 128:256] / AREA - m * m + FLOOR
        av[0, i] = lax.rsqrt(var)
        bv[0, i] = m

    moments(lambda j: hs[1, j], 0, NJ, xmom)

    def view_moments(v, carry):
        moments(lambda j: xs[v + 1, j], 0, NJ, lmom)
        finish(NM * 8, v)

        for i in range(NM):
            rows = slice(8 * i, 8 * i + 8)
            m = cmom[rows, 0:128] / AREA
            var = cmom[rows, 128:256] / AREA - m * m + FLOOR
            inv = lax.rsqrt(var) / SRC
            av[v + 1, i] = inv / AREA
            bv[v + 1, i] = m * inv
        return carry

    lax.fori_loop(0, SRC, view_moments, 0)

    lane = lax.broadcasted_iota(jnp.int32, (8, 128), 1)
    masks = [lane < HL * (v + 1) for v in range(SRC - 1)]

    def level(step, carry):
        starts = []
        for u in range(LB):
            l = LB * step + u
            begins = [SHIFT - ids[v] * l for v in range(SRC)]
            starts.append((l, begins))
            pieces = [hs[1, pl.ds(begins[v], NK)] for v in range(SRC)]
            prods = []
            for k in range(NK):
                piece = pieces[3][k]
                for v in (2, 1, 0):
                    piece = jnp.where(masks[v], pieces[v][k], piece)
                prods.append(hs[0, SHIFT + k] * piece)
            part = pl.ds(256 * u, 256)
            put_parts(lx.at[part], window11(prods), (0, 128))
            for v in range(SRC):
                moved = xs[v + 1, pl.ds(begins[v], NK)]
                prods = [xs[0, SHIFT + k] * moved[k] for k in range(NK)]
                put_parts(lhs.at[v // 2, part], window11(prods), (128 * (v % 2), 256 + 128 * (v % 2)))
        for p in range(SRC // 2):
            total = jnp.dot(lhs[p, :, 0:256], rt[...], preferred_element_type=f32)
            total += jnp.dot(lhs[p, :, 256:512], rt[...], preferred_element_type=f32)
            total += jnp.dot(lx[...], rx3[p], preferred_element_type=f32)
            yy[p] = total
        for u in range(LB):
            l, begins = starts[u]
            scale = [av[v + 1, pl.ds(begins[v], SEG)] for v in range(SRC)]
            shift = [bv[v + 1, pl.ds(begins[v], SEG)] for v in range(SRC)]
            for i in range(SEG):
                rows = slice(256 * u + 8 * i, 256 * u + 8 * i + 8)
                acc = None
                sub = None
                for v in range(SRC):
                    y = yy[v // 2, rows, 128 * (v % 2):128 * (v % 2) + 128]
                    a = y * scale[v][i]
                    s = shift[v][i]
                    acc = a if acc is None else acc + a
                    sub = s if sub is None else sub + s
                vol[l, i] = av[0, i] * (acc - bv[0, i] * sub)
        return carry

    lax.fori_loop(0, LEVELS // LB, level, 0)

    for role, rows, target, kind in kinds:
        there = side_there if kind else col >= 0

        @pl.when(role)
        def _(rows=rows, target=target, kind=kind):
            coarse_own(rows, target).wait()

        @pl.when(jnp.logical_not(role) & there)
        def _(rows=rows, target=target, kind=kind):
            coarse_copy(col, rows, target, kind).wait_recv()

    @pl.when(jnp.logical_not(side_there))
    def _():
        side_dst[...] = jnp.zeros(side_dst.shape, f32)

    up[...] = upsampled_tile(cb, row_mat, col_mat, *coarse_shape)

    def pick(i, carry):
        rows = pl.ds(pl.multiple_of(8 * i, 8), 8)
        codes = ht[rows, :]
        centre = up[rows, :]
        num = jnp.zeros((8, 128), f32)
        den = jnp.zeros((8, 128), f32)
        for k in range(HYP):
            table = [vol[l, i] for l in range(LEVELS)]
            for bit in range(4):
                odd = (codes & jnp.int32((1 << (4 * k + bit)) - (1 << 32 if 4 * k + bit == 31 else 0))) != 0
                table = [jnp.where(odd, table[t + 1], table[t]) for t in range(0, len(table), 2)]
            gain = 10.0 * table[0] - 10.0
            sel[k, rows, :] = gain
            cand = (lax.shift_right_logical(codes, 4 * k) & 15).astype(f32)
            d = cand - centre
            w = jnp.exp(gain - 0.1 * (d * d))
            num += w * cand
            den += w
        red[rows, :] = num / den
        return carry

    lax.fori_loop(0, SEG, pick, 0)


    lane = lax.broadcasted_iota(jnp.int32, (8, 128), 1)
    edge = jnp.zeros((8, 128), f32)
    for i in range(SEG):
        v = red[8 * i:8 * i + 8, :]
        edge = jnp.where(lane == i, jnp.broadcast_to(v[:, 0:1], (8, 128)), edge)
        edge = jnp.where(lane == SEG + i, jnp.broadcast_to(v[:, 127:128], (8, 128)), edge)
    border[...] = edge


    copies.clear()
    copies.extend(halos)
    push(0, 1, red.at[pl.ds(8 * SEG - 8, 8), :], near.at[2])
    push(0, -1, red.at[pl.ds(0, 8), :], near.at[3])
    push(1, 0, border, near.at[0])
    push(-1, 0, border, near.at[1])
    final = copies[len(halos):]

    leave(halos)
    for role, rows, target, kind in kinds:
        @pl.when(role)
        def _(rows=rows, target=target, kind=kind):
            def one(j, carry):
                @pl.when(j != col)
                def _():
                    coarse_copy(j, rows, target, kind).wait_send()

                return carry

            lax.fori_loop(0, nc, one, 0)

    arrive(final)
    lane = lax.broadcasted_iota(jnp.int32, (8, 128), 1)
    seg = lax.broadcasted_iota(jnp.int32, (8, 128), 0)
    row_edge = jnp.where((lane == 0) & (row == 0), 1.0, 0.0) + jnp.where(
        (lane == ROWS - 1) & (row == nr - 1), 1.0, 0.0)
    above_v = near[0]
    below_v = near[1]
    left, right = near.at[2], near.at[3]
    for i in range(SEG):
        rows = slice(8 * i, 8 * i + 8)
        r = red[rows, :]
        u = up[rows, :]
        h = ht[rows, :]
        north = jnp.where(lane == 0, jnp.broadcast_to(above_v[:, SEG + i:SEG + i + 1], (8, 128)), pltpu.roll(r, 1, 1))
        south = jnp.where(lane == ROWS - 1, jnp.broadcast_to(below_v[:, i:i + 1], (8, 128)), pltpu.roll(r, ROWS - 1, 1))
        if i == 0:
            west = jnp.concatenate([left[7:8, :], red[8 * SEG - 8:8 * SEG - 1, :]], axis=0)
        else:
            west = red[8 * i - 8:8 * i, :]
        if i == SEG - 1:
            east = jnp.concatenate([red[1:8, :], right[0:1, :]], axis=0)
        else:
            east = red[8 * i + 8:8 * i + 16, :]
        count = 4.0 - row_edge
        if i == 0:
            count = count - jnp.where((seg == 0) & (col == 0), 1.0, 0.0)
        if i == SEG - 1:
            count = count - jnp.where((seg == 7) & (col == nc - 1), 1.0, 0.0)
        centre = 0.5 * u + 0.5 * (north + south + west + east) / count
        num = jnp.zeros((8, 128), f32)
        den = jnp.zeros((8, 128), f32)
        for k in range(HYP):
            cand = (lax.shift_right_logical(h, 4 * k) & 15).astype(f32)
            d = cand - centre
            w = jnp.exp(sel[k, rows, :] - 0.1 * (d * d))
            num += w * cand
            den += w
        even = ((lane + i) & 1) == 0
        tmp[pl.ds(i, SEGS, stride=SEG), :] = jnp.where(even, r, num / den)
    out[...] = tmp[...].T
    leave(final)


def on_device(reference_image, source_images, hypotheses, source_ids, coarse_disp, coarse_conf):
    shape = (coarse_disp.shape[0] * lax.axis_size("col"), coarse_disp.shape[1])
    anywhere = pl.BlockSpec(memory_space=pltpu.HBM)
    n = SEG * 8
    return pl.pallas_call(
        functools.partial(stereo_kernel, shape),
        out_shape=jax.ShapeDtypeStruct((ROWS, COLS), f32),
        in_specs=[pl.BlockSpec(memory_space=pltpu.SMEM)] + [anywhere] * 5,
        out_specs=pl.BlockSpec(memory_space=pltpu.VMEM),
        scratch_shapes=[
            pltpu.VMEM((SRC + 1, ROWS, COLS), f32),
            pltpu.VMEM((HYP, ROWS, COLS), jnp.int32),
            pltpu.VMEM((2,) + coarse_disp.shape, f32),
            pltpu.VMEM((SRC + 1, CI, 128), f32),
            pltpu.VMEM((2, SRC + 1, 8, 512), f32),
            pltpu.VMEM((2, 32, min(256, coarse_disp.shape[1])), f32),
            pltpu.VMEM((n, 128), jnp.int32),
            pltpu.VMEM((COLS, ROWS), jnp.int32),
            pltpu.VMEM((HYP, n, 128), f32),
            pltpu.VMEM((n, 128), f32),
            pltpu.VMEM((n, 128), f32),
            pltpu.VMEM((8, 128), f32),
            pltpu.VMEM((COLS, ROWS), f32),
            pltpu.VMEM((4, 8, 128), f32),
            pltpu.VMEM((SRC + 1, NJ, 8, 128), f32),
            pltpu.VMEM((2, NJ, 8, 128), f32),
            pltpu.VMEM((256, 256), bf16),
            pltpu.VMEM((2, 256, 256), bf16),
            pltpu.VMEM((SRC, 256, 256), bf16),
            pltpu.VMEM((NM * 8 + 8, 768), bf16),
            pltpu.VMEM((NM * 8 + 8, 768), bf16),
            pltpu.VMEM((NM * 8, 256), f32),
            pltpu.VMEM((SRC + 1, NM, 8, 128), f32),
            pltpu.VMEM((SRC + 1, NM, 8, 128), f32),
            pltpu.VMEM((2, LB * n, 512), bf16),
            pltpu.VMEM((LB * n, 256), bf16),
            pltpu.VMEM((2, LB * n, 256), f32),
            pltpu.VMEM((LEVELS, SEG, 8, 128), f32),
            pltpu.VMEM((512, 128), f32),
            pltpu.VMEM((ROWS, 32), bf16),
            pltpu.VMEM((COLS, min(256, coarse_disp.shape[1])), bf16),
            pltpu.SemaphoreType.DMA((5,)),
            pltpu.SemaphoreType.DMA((1,)),
            pltpu.SemaphoreType.DMA((13,)),
            pltpu.SemaphoreType.DMA((13,)),
            pltpu.SemaphoreType.DMA((16,)),
            pltpu.SemaphoreType.DMA((2,)),
        ],
        compiler_params=pltpu.CompilerParams(
            collective_id=0, has_side_effects=True, vmem_limit_bytes=VMEM_LIMIT),
    )(source_ids, reference_image, source_images, hypotheses, coarse_disp, coarse_conf)


def solution(mesh):
    in_specs = (
        P("row", "col"),
        P(None, "row", "col"),
        P(None, "row", "col"),
        P(),
        P("col", None),
        P("col", None),
    )
    return jax.shard_map(
        on_device, mesh=mesh, in_specs=in_specs, out_specs=P("row", "col"), check_vma=False
    )
```
